256 devices in a mesh: clip: 32 (over z_lo, y, core), row: 2 (over z_hi), src: 4 (over x).
Axes of the slice: x: 4, y: 4, z: 8 (z_hi: 2, z_lo: 4; z = z_hi * 4 + z_lo), core: 2. Of those that a mesh axis runs over, the one named last changes fastest.
Arguments:
- mask_clip: bfloat16 [131072, 4096], P(('clip', 'row'), 'src'), parts along dimension 0, may hold values from -6 to 6
- source_shifts: int32 [16, 2], P('src'), may hold values from -64 to 64
- source_weights: int32 [16], P('src'), may hold values from 1 to 8
Outputs:
- intensity: float32 [32768, 1024], P(('clip', 'row', 'src')), parts along dimension 0
The draws below stay inside these ranges and needn't reach their ends.
There are 32 independent parts, one for each index of `clip`. The reference program is written for one: setup_inputs(seed, part) draws one part's arguments, and reference() takes and returns one part's arrays. A program takes and returns all parts, laid end to end along the dimension named above; an argument that names none is the same for every part. Nothing has to cross between parts.
All inputs are finite; a program needn't handle non-finite values.
Results may differ from the reference program's by a relative error of at most 0.0052.
Values may be sent and summed in bfloat16 or wider, within the bound.
No kernel may reach another device: no remote copies, remote signals or barrier semaphores. Data moves between devices by JAX's collectives and lax.ppermute only.
A program may use at most 64 MiB of HBM per device.

```python
import math
import jax
import jax.numpy as jnp
from jax import lax

NM = 4096
P_SIZE = 256
NI = 1024
SOURCES = 16
N_ROW = 2
N_SRC = 4


def with_ends(values, rng, least, top_value):
    place = [jax.random.randint(jax.random.fold_in(rng, axis), (), 0, length) for axis, length in enumerate(values.shape)]
    longest = values.shape.index(max(values.shape))
    neighbour = place[:longest] + [(place[longest] + 1) % values.shape[longest]] + place[longest + 1:]
    return values.at[tuple(place)].set(least).at[tuple(neighbour)].set(top_value)


def shard_levels(stream_key, extent, shards, smallest, top_value):
    loudness, own = 1.0, jax.random.fold_in(stream_key, 6)
    for dim, blocks in shards:
        heights = jnp.exp(jax.random.uniform(jax.random.fold_in(own, dim), (blocks,), jnp.float32, smallest / len(shards), top_value / len(shards)))
        loudness = loudness * jnp.repeat(heights, extent[dim] // blocks).reshape([-1 if axis == dim else 1 for axis in range(len(extent))])
    return loudness


def centred(stream_key, shape, scale, limit, cuts=(), held_as=jnp.bfloat16):
    drawn = scale * jax.random.normal(stream_key, shape, jnp.float32)
    if cuts:
        drawn = drawn * shard_levels(stream_key, shape, cuts, -0.22, 0.18)
    return jnp.clip(drawn, -limit, limit).astype(held_as)


def setup_inputs(seed: int = 0, part: int = 0) -> dict:
    keys = jax.random.split(jax.random.key(seed), 4)
    part_splits = jax.random.split(jax.random.fold_in(keys[3], part), 4)
    return {
        "mask_clip": centred(part_splits[0], (NM, NM), 1.0, 6.0, ((0, 2), (1, 4))),
        "source_shifts": with_ends(jax.random.randint(keys[1], (SOURCES, 2), 0 - P_SIZE // 4, P_SIZE // 4 + 1), jax.random.fold_in(keys[1], 1), 0 - P_SIZE // 4, (P_SIZE // 4 + 1) - 1).astype(jnp.int32),
        "source_weights": with_ends(jax.random.randint(keys[2], (SOURCES,), 1, 9), jax.random.fold_in(keys[2], 1), 1, 8).astype(jnp.int32),
    }


def twiddles(positions, length, scaling):
    frequency = jnp.arange(P_SIZE, dtype=jnp.int32) - P_SIZE // 2
    product = jnp.mod(positions[:, None] * frequency[None, :], length)
    angles = product.astype(jnp.float32) * jnp.float32(2.0 * math.pi / length)
    return (jnp.cos(angles) * jnp.float32(scaling), jnp.sin(angles) * jnp.float32(scaling))

def tile_spectrum(mask_tile, row_first, col_first):
    row_index = row_first + jnp.arange(mask_tile.shape[0], dtype=jnp.int32)
    col_index = col_first + jnp.arange(mask_tile.shape[1], dtype=jnp.int32)
    col_cos, col_sin = twiddles(col_index, NM, 1.0 / math.sqrt(NM))
    col_table = jnp.concatenate([col_cos, -col_sin], 1).astype(jnp.bfloat16)
    half_way = jnp.dot(mask_tile, col_table, preferred_element_type=jnp.float32).astype(jnp.bfloat16)
    row_cos, row_sin = twiddles(row_index, NM, 1.0 / math.sqrt(NM))
    row_table = jnp.concatenate([row_cos, row_sin], 1).T.astype(jnp.bfloat16)
    blocks = jnp.dot(row_table, half_way, preferred_element_type=jnp.float32)
    real_part = blocks[:P_SIZE, :P_SIZE] + blocks[P_SIZE:, P_SIZE:]
    imag_part = blocks[:P_SIZE, P_SIZE:] - blocks[P_SIZE:, :P_SIZE]
    return jnp.stack([real_part, imag_part])

def build_left(image_rows):
    row_cos, row_sin = twiddles(image_rows, NI, 1.0 / math.sqrt(P_SIZE))
    return jnp.concatenate([row_cos, row_sin], 0).astype(jnp.bfloat16)

def build_right():
    col_cos, col_sin = twiddles(jnp.arange(NI, dtype=jnp.int32), NI, 1.0 / math.sqrt(P_SIZE))
    upper = jnp.concatenate([col_cos.T, col_sin.T], 1)
    lower = jnp.concatenate([-col_sin.T, col_cos.T], 1)
    return jnp.concatenate([upper, lower], 0).astype(jnp.bfloat16)

def source_image(spectrum, shift_pair, weight, left_table, right_table):
    frequency = jnp.arange(P_SIZE, dtype=jnp.int32) - P_SIZE // 2
    along_rows = frequency + shift_pair[0]
    along_cols = frequency + shift_pair[1]
    radius = P_SIZE // 4
    inside = along_rows[:, None] * along_rows[:, None] + along_cols[None, :] * along_cols[None, :] <= radius * radius
    pupil_mask = inside.astype(jnp.bfloat16)
    passed = jnp.concatenate([spectrum[0] * pupil_mask, spectrum[1] * pupil_mask], 1)
    blocks = jnp.dot(left_table, passed, preferred_element_type=jnp.float32)
    row_count = left_table.shape[0] // 2
    k_real = blocks[:row_count, :P_SIZE] - blocks[row_count:, P_SIZE:]
    k_imag = blocks[:row_count, P_SIZE:] + blocks[row_count:, :P_SIZE]
    partial_value = jnp.concatenate([k_real, k_imag], 1).astype(jnp.bfloat16)
    field_pair = jnp.dot(partial_value, right_table, preferred_element_type=jnp.float32)
    field_real = field_pair[:, :NI]
    field_imag = field_pair[:, NI:]
    return weight.astype(jnp.float32) * (field_real * field_real + field_imag * field_imag)

def reference(mask_clip, source_shifts, source_weights):
    strip_rows = NM // N_ROW
    strip_cols = NM // N_SRC
    running_sum = jnp.zeros((2, P_SIZE, P_SIZE), jnp.float32)
    for strip_row in range(N_ROW):
        for strip_col in range(N_SRC):
            mask_tile = mask_clip[strip_row * strip_rows:(strip_row + 1) * strip_rows, strip_col * strip_cols:(strip_col + 1) * strip_cols]
            running_sum = running_sum + tile_spectrum(mask_tile, strip_row * strip_rows, strip_col * strip_cols)
    spectrum = running_sum.astype(jnp.bfloat16)
    left_table = build_left(jnp.arange(NI, dtype=jnp.int32))
    right_table = build_right()

    def add_source(running, source_item):
        shift_pair, weight = source_item
        return (running + source_image(spectrum, shift_pair, weight, left_table, right_table), None)
    summed, _ = lax.scan(add_source, jnp.zeros((NI, NI), jnp.float32), (source_shifts, source_weights))
    return summed / jnp.float32(SOURCES)
```

```python
import math

import jax
import jax.numpy as jnp
import numpy as np
from jax import lax
from jax.experimental import pallas as pl
from jax.experimental.pallas import tpu as pltpu
from jax.sharding import PartitionSpec as P

NM = 4096
NI = 1024
HALF = 128
BLOCK = 512
NT = (((1,), (1,)), ((), ()))
F32 = jnp.float32
BF16 = jnp.bfloat16


def forward_tables():
    freq = np.arange(HALF)
    pos = np.arange(NM // 4)
    angle = 2.0 * np.pi * ((freq[:, None] * pos[None, :]) % NM) / NM
    edge = 2.0 * np.pi * ((HALF * pos) % NM) / NM
    table = np.zeros((272, NM // 4), np.float64)
    table[:HALF] = np.cos(angle)
    table[HALF:256] = np.sin(angle)
    table[256] = np.cos(edge)
    table[257] = np.sin(edge)
    pattern = np.zeros((16, HALF), np.float64)
    pattern[2] = np.cos(edge[:HALF])
    pattern[3] = np.sin(edge[:HALF])
    return (table / 64).astype(np.float32), (pattern / 64).astype(np.float32)


def signed_frequencies():
    freq = np.concatenate([np.arange(HALF), -np.arange(HALF)])
    freq[HALF] = -HALF
    return freq


def inverse_tables():
    freq = signed_frequencies()
    rows = np.arange(NI)
    angle = 2.0 * np.pi * ((rows[:, None] * freq[None, :]) % NI) / NI
    left = np.stack([np.cos(angle), np.sin(angle)]).reshape(2, 8, HALF, 256)
    left = left.transpose(1, 0, 2, 3).reshape(8, 256, 256) / 16
    cos_y, sin_y = np.cos(angle).T / 16, np.sin(angle).T / 16
    right = np.stack([np.concatenate([cos_y, -sin_y], 0), np.concatenate([sin_y, cos_y], 0)])
    return left.astype(np.float32), right.astype(np.float32)


def quarter(turns):
    q = jnp.bitwise_and(turns, 3)
    cos_q = jnp.where(q == 0, 1.0, jnp.where(q == 2, -1.0, 0.0)).astype(F32)
    sin_q = jnp.where(q == 1, 1.0, jnp.where(q == 3, -1.0, 0.0)).astype(F32)
    return cos_q, sin_q


def forward_kernel(shifts, weights, mask, table, pattern, out, acc, acc_edge):
    step = pl.program_id(0)
    part = step // 2
    block = mask[...]
    half_way = lax.dot_general(block, table[:256, :], NT, preferred_element_type=F32).astype(BF16)
    folded = block[:, :HALF].astype(F32)
    for tile in range(1, 8):
        folded = folded + block[:, tile * HALF:(tile + 1) * HALF].astype(F32)
    folded = folded.astype(BF16)
    columns = pl.ds(pl.multiple_of((step % 2) * BLOCK, BLOCK), BLOCK)
    rows = table[:, columns]
    first = jnp.dot(rows, half_way, preferred_element_type=F32)
    second = jnp.dot(rows[:256], folded, preferred_element_type=F32)

    @pl.when(step % 2 == 0)
    def _():
        acc[part] = first
        acc_edge[part] = second

    @pl.when(step % 2 == 1)
    def _():
        acc[part] += first
        acc_edge[part] += second

    @pl.when(step == 3)
    def _():
        row_id = lax.axis_index("row")
        src_id = lax.axis_index("src")
        f_col = lax.broadcasted_iota(jnp.int32, (HALF, 256), 0)
        cos_q, sin_q = quarter(f_col)
        sign, _ = quarter(f_col * 2 * row_id)

        def join_rows(a, b, width):
            c, s, g = cos_q[:, :width], sin_q[:, :width], sign[:, :width]
            top = (a[:HALF] + c * b[:HALF] - s * b[HALF:256]) * g
            low = (a[HALF:256] + c * b[HALF:256] + s * b[:HALF]) * g
            return top, low

        def turn_columns(x):
            g_row = lax.broadcasted_iota(jnp.int32, (x.shape[0], HALF), 1)
            c, s = quarter(g_row * src_id)
            return c * x[:, :HALF] - s * x[:, HALF:], c * x[:, HALF:] + s * x[:, :HALF]

        a, b = acc[0], acc[1]
        top, low = join_rows(a, b, 256)
        for start, x in ((0, top), (HALF, low)):
            x_cos, x_sin = turn_columns(x)
            out[start:start + HALF, :HALF] = x_cos.astype(BF16)
            out[start:start + HALF, HALF:] = x_sin.astype(BF16)
        e_cos, e_sin = turn_columns(a[256:] + b[256:])
        edge_top, edge_low = join_rows(acc_edge[0], acc_edge[1], HALF)
        edges = jnp.concatenate([edge_top, edge_low], 0).astype(BF16)
        crossed = lax.dot_general(pattern[...], edges, NT, preferred_element_type=F32)
        row = lax.broadcasted_iota(jnp.int32, (16, HALF), 0)
        e_cos = e_cos + crossed[:, :HALF]
        e_sin = e_sin + crossed[:, HALF:]
        shift_f = jnp.zeros((16, HALF), F32)
        shift_g = jnp.zeros((16, HALF), F32)
        for i in range(4):
            w = weights[i].astype(F32)
            here = row == 4 + src_id * 2 + i // 2
            if i % 2 == 0:
                e_cos = jnp.where(here, w, e_cos)
            else:
                e_sin = jnp.where(here, w, e_sin)
            mine = row == src_id * 4 + i
            shift_f = jnp.where(mine, shifts[i, 0].astype(F32), shift_f)
            shift_g = jnp.where(mine, shifts[i, 1].astype(F32), shift_g)
        out[256:272, :HALF] = e_cos.astype(BF16)
        out[256:272, HALF:] = e_sin.astype(BF16)
        out[272:288, :HALF] = shift_f.astype(BF16)
        out[272:288, HALF:] = shift_g.astype(BF16)


def forward(mask_clip, shifts, weights, table, pattern):
    return pl.pallas_call(
        forward_kernel,
        grid=(4,),
        in_specs=[
            pl.BlockSpec(memory_space=pltpu.SMEM),
            pl.BlockSpec(memory_space=pltpu.SMEM),
            pl.BlockSpec((BLOCK, NM // 4), lambda i: (i, 0)),
            pl.BlockSpec((272, NM // 4), lambda i: (0, 0)),
            pl.BlockSpec((16, HALF), lambda i: (0, 0)),
        ],
        out_specs=pl.BlockSpec((288, 256), lambda i: (0, 0)),
        out_shape=jax.ShapeDtypeStruct((288, 256), BF16),
        scratch_shapes=[pltpu.VMEM((2, 272, 256), F32), pltpu.VMEM((2, 256, HALF), F32)],
        compiler_params=pltpu.CompilerParams(vmem_limit_bytes=60 * 1024 * 1024),
        cost_estimate=pl.CostEstimate(flops=1_700_000_000, bytes_accessed=5_000_000, transcendentals=0),
        name="forward",
    )(shifts, weights, mask_clip, table, pattern)


def inverse_kernel(mine, other, left, right, out, spec, fields):
    total = mine[:256].astype(F32) + other[:256].astype(F32)
    cc, cs = total[:HALF, :HALF], total[:HALF, HALF:]
    sc, ss = total[HALF:, :HALF], total[HALF:, HALF:]
    edge = mine[256:272].astype(F32) + other[256:272].astype(F32)
    rc, rs = edge[0:1], edge[1:2]
    xc, xs = edge[2:3], edge[3:4]
    row_re = (rc[:, :HALF] + rs[:, HALF:], rc[:, :HALF] - rs[:, HALF:])
    row_im = (rs[:, :HALF] - rc[:, HALF:], rs[:, :HALF] + rc[:, HALF:])
    col_re = jnp.concatenate([xc[:, :HALF] + xs[:, HALF:], xc[:, :HALF] - xs[:, HALF:]], 1)
    col_im = jnp.concatenate([xs[:, :HALF] - xc[:, HALF:], xs[:, :HALF] + xc[:, HALF:]], 1)
    first_row = lax.broadcasted_iota(jnp.int32, (HALF, HALF), 0) == 0
    first_lane = lax.broadcasted_iota(jnp.int32, (HALF, HALF), 1) == 0

    def stand(row):
        return jnp.broadcast_to(row, (HALF, HALF)).T

    quads = {
        (0, 0): (cc - ss, -(sc + cs)),
        (0, 1): (cc + ss, cs - sc),
        (1, 0): (cc + ss, sc - cs),
        (1, 1): (cc - ss, sc + cs),
    }
    for (i, j), (re, im) in quads.items():
        if i == 1:
            re = jnp.where(first_row, row_re[j], re)
            im = jnp.where(first_row, row_im[j], im)
        if j == 1:
            re = jnp.where(first_lane, stand(col_re[:, i * HALF:(i + 1) * HALF]), re)
            im = jnp.where(first_lane, stand(col_im[:, i * HALF:(i + 1) * HALF]), im)
        spec[i * HALF:(i + 1) * HALF, j * HALF:(j + 1) * HALF] = re.astype(BF16)
        spec[i * HALF:(i + 1) * HALF, 256 + j * HALF:256 + (j + 1) * HALF] = im.astype(BF16)

    shifts = mine[272:288].astype(F32)
    loads = jnp.sqrt(mine[256:272].astype(F32)) * 0.25
    f_low = lax.broadcasted_iota(jnp.int32, (HALF, HALF), 0)
    g_low = lax.broadcasted_iota(jnp.int32, (1, HALF), 1)
    f_halves = (f_low.astype(F32), jnp.where(f_low == 0, -HALF, -f_low).astype(F32))
    g_halves = (g_low.astype(F32), jnp.where(g_low == 0, -HALF, -g_low).astype(F32))
    zero = jnp.zeros((HALF, HALF), BF16)
    for s in range(16):
        a, b = shifts[s:s + 1, :HALF], shifts[s:s + 1, HALF:]
        w = loads[4 + s // 2:5 + s // 2, (s % 2) * HALF:(s % 2 + 1) * HALF]
        room = [4096.0 - (f + a) * (f + a) for f in f_halves]
        reach = [(g + b) * (g + b) for g in g_halves]
        inside = [[r >= q for q in reach] for r in room]
        passed = jnp.concatenate(
            [
                jnp.concatenate(
                    [
                        jnp.where(
                            inside[i][j % 2],
                            spec[i * HALF:(i + 1) * HALF, j * HALF:(j + 1) * HALF],
                            zero,
                        )
                        for j in range(4)
                    ],
                    1,
                )
                for i in range(2)
            ],
            0,
        )
        blocks = jnp.dot(left[...], passed, preferred_element_type=F32)
        w2 = jnp.concatenate([w, w], 1)
        k_re = (blocks[:HALF, :256] - blocks[HALF:, 256:]) * w2
        k_im = (blocks[:HALF, 256:] + blocks[HALF:, :256]) * w2
        fields[s * HALF:(s + 1) * HALF, :256] = k_re.astype(BF16)
        fields[s * HALF:(s + 1) * HALF, 256:] = k_im.astype(BF16)
    for chunk in range(4):
        span = slice(chunk * 256, (chunk + 1) * 256)
        summed = jnp.zeros((HALF, 256), F32)
        for group in range(4):
            k = fields[group * 512:(group + 1) * 512, :]
            e_re = jnp.dot(k, right[0, :, span], preferred_element_type=F32)
            e_im = jnp.dot(k, right[1, :, span], preferred_element_type=F32)
            power = e_re * e_re + e_im * e_im
            for i in range(4):
                summed = summed + power[i * HALF:(i + 1) * HALF]
        out[:, span] = summed


def inverse(mine, other, left, right):
    vmem = pl.BlockSpec(memory_space=pltpu.VMEM)
    return pl.pallas_call(
        inverse_kernel,
        in_specs=[vmem] * 4,
        out_specs=vmem,
        out_shape=jax.ShapeDtypeStruct((HALF, NI), F32),
        scratch_shapes=[pltpu.VMEM((256, 512), BF16), pltpu.VMEM((2048, 512), BF16)],
        compiler_params=pltpu.CompilerParams(vmem_limit_bytes=24 * 1024 * 1024),
        cost_estimate=pl.CostEstimate(flops=5_400_000_000, bytes_accessed=3_000_000, transcendentals=0),
        name="inverse",
    )(mine, other, left, right)


def body(mask_clip, source_shifts, source_weights):
    table, pattern = forward_tables()
    left, right = inverse_tables()
    place = lax.axis_index("row") * 4 + lax.axis_index("src")
    left_mine = lax.dynamic_index_in_dim(jnp.asarray(left, BF16), place, 0, keepdims=False)
    partial_sum = forward(
        mask_clip, source_shifts, source_weights, jnp.asarray(table, BF16), jnp.asarray(pattern, BF16)
    )
    summed = partial_sum.astype(F32)
    for k in (1, 2, 3):
        summed = summed + lax.ppermute(partial_sum, "src", [(i, (i + k) % 4) for i in range(4)]).astype(F32)
    summed = summed.astype(BF16)
    other = lax.ppermute(summed, "row", [(0, 1), (1, 0)])
    return inverse(summed, other, left_mine, jnp.asarray(right, BF16))


def solution(mesh):
    placed = (P(("clip", "row"), "src"), P("src", None), P("src"))
    return jax.shard_map(
        body, mesh=mesh, in_specs=placed, out_specs=P(("clip", "row", "src"), None), check_vma=False
    )
```

```python
import jax
import jax.numpy as jnp
import numpy as np
from jax import lax
from jax.experimental import pallas as pl
from jax.experimental.pallas import tpu as pltpu
from jax.sharding import PartitionSpec as P

NM = 4096
NI = 1024
TILE = NM // 4
HALF = 128
CHUNKS = ((0, 512), (512, 1024), (1024, 2048))
COARSE = 256
NT = (((1,), (1,)), ((), ()))
F32 = jnp.float32
BF16 = jnp.bfloat16
VMEM = pl.BlockSpec(memory_space=pltpu.VMEM)


def forward_tables():
    freq = np.arange(HALF)
    pos = np.arange(TILE)
    angle = 2.0 * np.pi * ((freq[:, None] * pos[None, :]) % NM) / NM
    edge = 2.0 * np.pi * ((HALF * pos) % NM) / NM
    table = np.zeros((272, TILE), np.float64)
    table[:HALF] = np.cos(angle)
    table[HALF:256] = np.sin(angle)
    table[256] = np.cos(edge)
    table[257] = np.sin(edge)
    table[266, :HALF] = np.cos(edge[:HALF])
    table[267, :HALF] = np.sin(edge[:HALF])
    return (table / 64).astype(np.float32)


def inverse_tables():
    freq = np.concatenate([np.arange(HALF), -np.arange(HALF)])
    freq[HALF] = -HALF
    rows = np.arange(NI)
    angle = 2.0 * np.pi * ((rows[:, None] * freq[None, :]) % NI) / NI
    left = [np.stack([np.cos(angle[:HALF] + t), np.sin(angle[:HALF] + t)]) / 16 for t in (0.0, np.pi / 4)]
    left = np.stack(left)
    cos_y, sin_y = np.cos(angle[::4]).T / 16, np.sin(angle[::4]).T / 16
    right = np.stack([np.concatenate([cos_y, -sin_y], 0), np.concatenate([sin_y, cos_y], 0)])
    j = np.arange(COARSE)
    harmonic = np.arange(1, HALF)
    columns = np.arange(NI)
    distance = (columns[None, :] - 4 * j[:, None]) % NI
    lags = 2.0 * np.pi * ((np.arange(NI)[:, None] * harmonic[None, :]) % NI) / NI
    wave = (1.0 + 2.0 * np.cos(lags).sum(1) + np.cos(2.0 * np.pi * (np.arange(NI) * HALF % NI) / NI)) / COARSE
    spread = wave[distance]
    high = np.asarray(spread.astype(np.float32).astype(BF16), np.float64)
    spread = np.stack([high, spread - high])
    sine = np.zeros((8, NI), np.float64)
    sine[0] = -2.0 * np.sin(np.pi * (columns % 8) / 4) / 256
    return tuple(x.astype(np.float32) for x in (left, right, spread, sine))


def quarter(turns):
    q = jnp.bitwise_and(turns, 3)
    cos_q = jnp.where(q == 0, 1.0, jnp.where(q == 2, -1.0, 0.0)).astype(F32)
    sin_q = jnp.where(q == 1, 1.0, jnp.where(q == 3, -1.0, 0.0)).astype(F32)
    return cos_q, sin_q


def forward_kernel(shifts_in, weights_in, mask, table_in, own, one, two, three,
                   shifts, weights, block, table, half_way, folded, whole, edge, sem):
    small_copies = [
        pltpu.make_async_copy(table_in, table, sem.at[0]),
        pltpu.make_async_copy(shifts_in, shifts, sem.at[1]),
        pltpu.make_async_copy(weights_in, weights, sem.at[2]),
    ]
    copies = [
        pltpu.make_async_copy(mask.at[start:stop], block.at[start:stop], sem.at[3 + i])
        for i, (start, stop) in enumerate(CHUNKS)
    ]
    for copy in (small_copies[0], *copies, *small_copies[1:]):
        copy.start()
    row_id = lax.axis_index("row")
    src_id = lax.axis_index("src")
    f_col = lax.broadcasted_iota(jnp.int32, (HALF, 256), 0)
    cos_f, sin_f = quarter(f_col)
    sign, _ = quarter(f_col * 2 * row_id)
    cos_g, sin_g = quarter(lax.broadcasted_iota(jnp.int32, (HALF, HALF), 1) * src_id)

    def join_rows(a, b):
        top = (a[:HALF] + cos_f * b[:HALF] - sin_f * b[HALF:256]) * sign
        low = (a[HALF:256] + cos_f * b[HALF:256] + sin_f * b[:HALF]) * sign
        return top, low

    def turn_columns(x):
        c, s = cos_g[:x.shape[0]], sin_g[:x.shape[0]]
        return c * x[:, :HALF] - s * x[:, HALF:], c * x[:, HALF:] + s * x[:, :HALF]

    small_copies[0].wait()
    sums = []
    for copy, (start, stop) in zip(copies, CHUNKS):
        copy.wait()
        part, at = start // TILE, start % TILE
        half_way[start:stop] = lax.dot_general(
            block[start:stop], table[:256, :], NT, preferred_element_type=F32
        ).astype(BF16)
        for low in range(0, stop - start, 64):
            rows = slice(start + low, start + low + 64)
            tiles = [block[rows, tile * HALF:(tile + 1) * HALF] for tile in range(8)]
            while len(tiles) > 1:
                tiles = [tiles[t] + tiles[t + 1] for t in range(0, len(tiles), 2)]
            folded[at + low:at + low + 64, part * HALF:(part + 1) * HALF] = tiles[0]
        if start == TILE:
            sums.append(jnp.dot(table[:264], half_way[:TILE], preferred_element_type=F32))
    sums.append(jnp.dot(table[:264], half_way[TILE:], preferred_element_type=F32))
    sides = jnp.dot(table[:256, :], folded[...], preferred_element_type=F32)
    for copy in small_copies[1:]:
        copy.wait()
    a, b = sums
    for start, x in zip((0, HALF), join_rows(a, b)):
        x_cos, x_sin = turn_columns(x)
        whole[start:start + HALF, :HALF] = x_cos
        whole[start:start + HALF, HALF:] = x_sin
    e_cos, e_sin = turn_columns(a[256:] + b[256:])
    s_a, s_b = sides[:, :HALF], sides[:, HALF:]
    c, s, g = cos_f[:, :HALF], sin_f[:, :HALF], sign[:, :HALF]
    edges = jnp.concatenate(
        [
            (s_a[:HALF] + c * s_b[:HALF] - s * s_b[HALF:]) * g,
            (s_a[HALF:] + c * s_b[HALF:] + s * s_b[:HALF]) * g,
        ],
        0,
    ).astype(BF16)
    crossed = lax.dot_general(table[264:272, :HALF], edges, NT, preferred_element_type=F32)
    edge[:, :HALF] = e_cos + crossed[:, :HALF]
    edge[:, HALF:] = e_sin + crossed[:, HALF:]
    row = lax.broadcasted_iota(jnp.int32, (8, HALF), 0)
    first = jnp.zeros((8, HALF), F32)
    second = jnp.zeros((8, HALF), F32)
    for i in range(4):
        first = jnp.where(row == 1 + i, shifts[0, i].astype(F32), first)
        second = jnp.where(row == 1 + i, shifts[1, i].astype(F32), second)
        w = weights[i].astype(F32)
        if i % 2 == 0:
            first = jnp.where(row == 5 + i // 2, w, first)
        else:
            second = jnp.where(row == 5 + i // 2, w, second)
    sources = jnp.concatenate([first, second], 1)
    row = lax.broadcasted_iota(jnp.int32, (8, 256), 0)
    for k, out in enumerate((own, one, two, three)):
        q = lax.rem(src_id + k, 4)
        low = pl.ds(pl.multiple_of(q * 32, 32), 32)
        high = pl.ds(pl.multiple_of(HALF + q * 32, 32), 32)
        out[:32] = whole[low].astype(BF16)
        out[32:64] = whole[high].astype(BF16)
        line = edge[pl.ds(q, 1)]
        out[64:72] = jnp.where(row == 0, line, sources if k == 0 else 0.0).astype(BF16)


def forward(mask_clip, shifts, weights, table):
    quarter_shape = jax.ShapeDtypeStruct((72, 256), BF16)
    hbm = pl.BlockSpec(memory_space=pltpu.HBM)
    return pl.pallas_call(
        forward_kernel,
        in_specs=[hbm] * 4,
        out_specs=[VMEM] * 4,
        out_shape=[quarter_shape] * 4,
        scratch_shapes=[
            pltpu.SMEM((2, 4), jnp.int32),
            pltpu.SMEM((4,), jnp.int32),
            pltpu.VMEM((2 * TILE, TILE), BF16),
            pltpu.VMEM((272, TILE), BF16),
            pltpu.VMEM((2 * TILE, 256), BF16),
            pltpu.VMEM((TILE, 256), BF16),
            pltpu.VMEM((256, 256), F32),
            pltpu.VMEM((8, 256), F32),
            pltpu.SemaphoreType.DMA((3 + len(CHUNKS),)),
        ],
        compiler_params=pltpu.CompilerParams(vmem_limit_bytes=16 * 1024 * 1024),
        cost_estimate=pl.CostEstimate(flops=1_700_000_000, bytes_accessed=5_000_000, transcendentals=0),
        name="forward",
    )(*[pltpu.with_memory_space_constraint(x, pltpu.HBM) for x in (shifts, weights, mask_clip, table)])


def add_kernel(own, one, two, three, out):
    out[...] = (
        own[...].astype(F32) + one[...].astype(F32) + two[...].astype(F32) + three[...].astype(F32)
    ).astype(BF16)


def finish_kernel(mine, other, out):
    total = mine[...].astype(F32) + other[...].astype(F32)
    cc, cs = total[:32, :HALF], total[:32, HALF:]
    sc, ss = total[32:64, :HALF], total[32:64, HALF:]
    out[:32, :HALF] = (cc - ss).astype(BF16)
    out[:32, HALF:] = (cc + ss).astype(BF16)
    out[32:64, :HALF] = -(sc + cs).astype(BF16)
    out[32:64, HALF:] = (cs - sc).astype(BF16)
    row = lax.broadcasted_iota(jnp.int32, (8, 256), 0)
    out[64:72] = jnp.where(row == 0, total[64:72], total[64:72] * 0.5).astype(BF16)


def small(kernel, name, *args):
    return pl.pallas_call(
        kernel,
        in_specs=[VMEM] * len(args),
        out_specs=VMEM,
        out_shape=jax.ShapeDtypeStruct((72, 256), BF16),
        compiler_params=pltpu.CompilerParams(vmem_limit_bytes=4 * 1024 * 1024),
        name=name,
    )(*args)


def inverse_kernel(c0, c1, c2, c3, left, right, spread, sine, out, spec, edge, fields):
    src_id = lax.axis_index("src")
    quarters = (c0, c1, c2, c3)
    for k, chunk in enumerate(quarters):
        q = lax.rem(src_id + 4 - k, 4)
        low = pl.ds(pl.multiple_of(q * 32, 32), 32)
        high = pl.ds(pl.multiple_of(HALF + q * 32, 32), 32)
        re, im = chunk[:32], chunk[32:64]
        spec[low, :256] = re
        spec[low, 256:] = im
        spec[high, :HALF] = re[:, HALF:]
        spec[high, HALF:256] = re[:, :HALF]
        spec[high, 256:384] = -im[:, HALF:]
        spec[high, 384:] = -im[:, :HALF]
        edge[pl.ds(q, 1)] = chunk[64:72].astype(F32)[0:1]
    rc, rs, xc, xs = (edge[i:i + 1] for i in range(4))
    first_row = jnp.concatenate(
        [
            rc[:, :HALF] + rs[:, HALF:],
            rc[:, :HALF] - rs[:, HALF:],
            rs[:, :HALF] - rc[:, HALF:],
            rs[:, :HALF] + rc[:, HALF:],
        ],
        1,
    )
    col_re = jnp.concatenate([xc[:, :HALF] + xs[:, HALF:], xc[:, :HALF] - xs[:, HALF:]], 1)
    col_im = jnp.concatenate([xs[:, :HALF] - xc[:, HALF:], xs[:, :HALF] + xc[:, HALF:]], 1)
    row = lax.broadcasted_iota(jnp.int32, (16, 512), 0)
    spec[HALF:HALF + 16] = jnp.where(
        row == 0, first_row, spec[HALF:HALF + 16].astype(F32)
    ).astype(BF16)
    first_lane = lax.broadcasted_iota(jnp.int32, (HALF, HALF), 1) == 0
    for i in range(2):
        rows = slice(i * HALF, (i + 1) * HALF)
        for line, lanes in ((col_re, slice(128, 256)), (col_im, slice(384, 512))):
            stood = jnp.broadcast_to(line[:, rows], (HALF, HALF)).T
            spec[rows, lanes] = jnp.where(first_lane, stood, spec[rows, lanes].astype(F32)).astype(BF16)

    f_low = lax.broadcasted_iota(jnp.int32, (HALF, HALF), 0)
    g_low = lax.broadcasted_iota(jnp.int32, (1, HALF), 1)
    f_halves = (f_low.astype(F32), jnp.where(f_low == 0, -HALF, -f_low).astype(F32))
    g_halves = (g_low.astype(F32), jnp.where(g_low == 0, -HALF, -g_low).astype(F32))
    g_all = jnp.concatenate(g_halves, 1)
    zero = jnp.zeros((HALF, HALF), BF16)
    ends = [jnp.zeros((1, 1), F32)]

    def propagate(s):
        info = quarters[s // 4][64:72].astype(F32)
        i = s % 4
        a, b = info[1 + i:2 + i, :HALF], info[1 + i:2 + i, HALF:]
        w = jnp.sqrt(info[5 + i // 2:6 + i // 2, (i % 2) * HALF:(i % 2 + 1) * HALF]) * 0.25
        room = [4096.0 - (f + a) * (f + a) for f in f_halves]
        reach = [(g + b) * (g + b) for g in g_halves]
        inside = [[r >= q for q in reach] for r in room]
        passed = jnp.concatenate(
            [
                jnp.concatenate(
                    [
                        jnp.where(
                            inside[i][j % 2],
                            spec[i * HALF:(i + 1) * HALF, j * HALF:(j + 1) * HALF],
                            zero,
                        )
                        for j in range(4)
                    ],
                    1,
                )
                for i in range(2)
            ],
            0,
        )
        blocks = jnp.dot(left[...], passed, preferred_element_type=F32)
        w2 = jnp.concatenate([w, w], 1)
        k_re = (blocks[:HALF, :256] - blocks[HALF:, 256:]) * w2
        k_im = (blocks[:HALF, 256:] + blocks[HALF:, :256]) * w2
        fields[s * HALF:(s + 1) * HALF, :256] = k_re.astype(BF16)
        fields[s * HALF:(s + 1) * HALF, 256:] = k_im.astype(BF16)
        at = g_all + jnp.concatenate([b, b], 1)
        r, m = k_re[0:1], k_im[0:1]
        pick = lambda x, v: jnp.sum(jnp.where(at == v, x, 0.0), axis=1, keepdims=True)
        ends[0] = ends[0] + pick(m, 64.0) * pick(r, -64.0) - pick(r, 64.0) * pick(m, -64.0)

    def power(group):
        k = fields[group * 512:(group + 1) * 512, :]
        e_re = jnp.dot(k, right[0], preferred_element_type=F32)
        e_im = jnp.dot(k, right[1], preferred_element_type=F32)
        p = e_re * e_re + e_im * e_im
        return (p[:HALF] + p[HALF:256]) + (p[256:384] + p[384:])

    summed = None
    for group in range(4):
        for s in range(4):
            propagate(group * 4 + s)
        if group:
            p = power(group - 1)
            summed = p if summed is None else summed + p
    summed = summed + power(3)
    high = summed.astype(BF16)
    low = (summed - high.astype(F32)).astype(BF16)
    tail = ends[0] * sine[0:1]
    out[...] = (
        jnp.dot(high, spread[0], preferred_element_type=F32)
        + jnp.dot(low, spread[0], preferred_element_type=F32)
        + jnp.dot(high, spread[1], preferred_element_type=F32)
        + tail
    )


def inverse(*args):
    return pl.pallas_call(
        inverse_kernel,
        in_specs=[VMEM] * len(args),
        out_specs=VMEM,
        out_shape=jax.ShapeDtypeStruct((HALF, NI), F32),
        scratch_shapes=[
            pltpu.VMEM((256, 512), BF16),
            pltpu.VMEM((8, 256), F32),
            pltpu.VMEM((2048, 512), BF16),
        ],
        compiler_params=pltpu.CompilerParams(vmem_limit_bytes=24 * 1024 * 1024),
        cost_estimate=pl.CostEstimate(flops=2_500_000_000, bytes_accessed=3_000_000, transcendentals=0),
        name="inverse",
    )(*args)


def place_rows(left, place):
    freq = jnp.arange(256, dtype=jnp.int32)
    freq = jnp.where(freq < HALF, freq, jnp.where(freq == HALF, -HALF, HALF - freq))
    eighths = freq * place
    cos_q, sin_q = (x.astype(BF16) for x in quarter(jnp.right_shift(eighths, 1)))
    base = jnp.where(jnp.bitwise_and(eighths, 1) == 1, left[1], left[0])
    return jnp.concatenate([base[0] * cos_q - base[1] * sin_q, base[1] * cos_q + base[0] * sin_q], 0)


def ring(x, k):
    return lax.ppermute(x, "src", [(i, (i + k) % 4) for i in range(4)])


def body(mask_clip, source_shifts, source_weights):
    table = forward_tables()
    left, right, spread, sine = inverse_tables()
    place = lax.axis_index("row") * 4 + lax.axis_index("src")
    left_mine = place_rows(jnp.asarray(left, BF16), place)
    parts = forward(mask_clip, source_shifts.T, source_weights, jnp.asarray(table, BF16))
    mine = small(add_kernel, "add", parts[0], *[ring(parts[k], k) for k in (1, 2, 3)])
    other = lax.ppermute(mine, "row", [(0, 1), (1, 0)])
    whole = small(finish_kernel, "finish", mine, other)
    return inverse(
        whole,
        *[ring(whole, k) for k in (1, 2, 3)],
        left_mine,
        jnp.asarray(right, BF16),
        jnp.asarray(spread, BF16),
        jnp.asarray(sine, F32),
    )


def solution(mesh):
    placed = (P(("clip", "row"), "src"), P("src", None), P("src"))
    return jax.shard_map(
        body, mesh=mesh, in_specs=placed, out_specs=P(("clip", "row", "src"), None), check_vma=False
    )
```

```python
import jax
import jax.numpy as jnp
import numpy as np
from jax import lax
from jax.experimental import pallas as pl
from jax.experimental.pallas import tpu as pltpu
from jax.sharding import PartitionSpec as P

NM = 4096
NI = 1024
TILE = NM // 4
HALF = 128
CHUNKS = ((0, 512), (512, 1024), (1024, 1536), (1536, 2048))
SENT = 272
SUMMED = 264
COARSE = 256
NT = (((1,), (1,)), ((), ()))
F32 = jnp.float32
BF16 = jnp.bfloat16
VMEM = pl.BlockSpec(memory_space=pltpu.VMEM)


def forward_tables():
    freq = np.arange(HALF)
    pos = np.arange(TILE)
    angle = 2.0 * np.pi * ((freq[:, None] * pos[None, :]) % NM) / NM
    edge = 2.0 * np.pi * ((HALF * pos) % NM) / NM
    table = np.zeros((272, TILE), np.float64)
    table[:HALF] = np.cos(angle)
    table[HALF:256] = np.sin(angle)
    table[256] = np.cos(edge)
    table[257] = np.sin(edge)
    table[266, :HALF] = np.cos(edge[:HALF])
    table[267, :HALF] = np.sin(edge[:HALF])
    return (table / 64).astype(np.float32)


def inverse_tables():
    freq = np.concatenate([np.arange(HALF), -np.arange(HALF)])
    freq[HALF] = -HALF
    rows = np.arange(NI)
    angle = 2.0 * np.pi * ((rows[:, None] * freq[None, :]) % NI) / NI
    left = [np.stack([np.cos(angle[:HALF] + t), np.sin(angle[:HALF] + t)]) / 16 for t in (0.0, np.pi / 4)]
    left = np.stack(left)
    cos_y, sin_y = np.cos(angle[::4]).T / 64, np.sin(angle[::4]).T / 64
    right = np.stack([np.concatenate([cos_y, -sin_y], 0), np.concatenate([sin_y, cos_y], 0)])
    j = np.arange(COARSE)
    harmonic = np.arange(1, HALF)
    columns = np.arange(NI)
    distance = (columns[None, :] - 4 * j[:, None]) % NI
    lags = 2.0 * np.pi * ((np.arange(NI)[:, None] * harmonic[None, :]) % NI) / NI
    wave = (1.0 + 2.0 * np.cos(lags).sum(1) + np.cos(2.0 * np.pi * (np.arange(NI) * HALF % NI) / NI)) / COARSE
    spread = wave[distance]
    high = np.asarray(spread.astype(np.float32).astype(BF16), np.float64)
    spread = np.stack([high, spread - high])
    sine = np.zeros((8, NI), np.float64)
    sine[0] = -2.0 * np.sin(np.pi * (columns % 8) / 4) / 4096
    return tuple(x.astype(np.float32) for x in (left, right, spread, sine))


def quarter(turns):
    q = jnp.bitwise_and(turns, 3)
    cos_q = jnp.where(q == 0, 1.0, jnp.where(q == 2, -1.0, 0.0)).astype(F32)
    sin_q = jnp.where(q == 1, 1.0, jnp.where(q == 3, -1.0, 0.0)).astype(F32)
    return cos_q, sin_q


def forward_kernel(shifts_in, weights_in, mask, table_in, out,
                   shifts, weights, block, table, half_way, folded, sem):
    small_copies = [
        pltpu.make_async_copy(table_in, table, sem.at[0]),
        pltpu.make_async_copy(shifts_in, shifts, sem.at[1]),
        pltpu.make_async_copy(weights_in, weights, sem.at[2]),
    ]
    copies = [
        pltpu.make_async_copy(mask.at[start:stop], block.at[start:stop], sem.at[3 + i])
        for i, (start, stop) in enumerate(CHUNKS)
    ]
    for copy in (small_copies[0], *copies, *small_copies[1:]):
        copy.start()
    row_id = lax.axis_index("row")
    src_id = lax.axis_index("src")
    f_col = lax.broadcasted_iota(jnp.int32, (HALF, 256), 0)
    cos_f, sin_f = quarter(f_col)
    sign, _ = quarter(f_col * 2 * row_id)
    cos_g, sin_g = quarter(lax.broadcasted_iota(jnp.int32, (HALF, HALF), 1) * src_id)

    def join_rows(a, b):
        top = (a[:HALF] + cos_f * b[:HALF] - sin_f * b[HALF:256]) * sign
        low = (a[HALF:256] + cos_f * b[HALF:256] + sin_f * b[:HALF]) * sign
        return top, low

    def turn_columns(x):
        c, s = cos_g[:x.shape[0]], sin_g[:x.shape[0]]
        return c * x[:, :HALF] - s * x[:, HALF:], c * x[:, HALF:] + s * x[:, :HALF]

    small_copies[0].wait()
    sums = []
    for copy, (start, stop) in zip(copies, CHUNKS):
        copy.wait()
        part, at = start // TILE, start % TILE
        half_way[start:stop] = lax.dot_general(
            block[start:stop], table[:256, :], NT, preferred_element_type=F32
        ).astype(BF16)
        for low in range(0, stop - start, 64):
            rows = slice(start + low, start + low + 64)
            tiles = [block[rows, tile * HALF:(tile + 1) * HALF] for tile in range(8)]
            while len(tiles) > 1:
                tiles = [tiles[t] + tiles[t + 1] for t in range(0, len(tiles), 2)]
            folded[at + low:at + low + 64, part * HALF:(part + 1) * HALF] = tiles[0]
        if start == TILE:
            sums.append(jnp.dot(table[:264], half_way[:TILE], preferred_element_type=F32))
    sums.append(jnp.dot(table[:264], half_way[TILE:], preferred_element_type=F32))
    sides = jnp.dot(table[:256, :], folded[...], preferred_element_type=F32)
    for copy in small_copies[1:]:
        copy.wait()
    a, b = sums
    for start, x in zip((0, HALF), join_rows(a, b)):
        x_cos, x_sin = turn_columns(x)
        out[start:start + HALF, :HALF] = x_cos.astype(BF16)
        out[start:start + HALF, HALF:] = x_sin.astype(BF16)
    e_cos, e_sin = turn_columns(a[256:] + b[256:])
    s_a, s_b = sides[:, :HALF], sides[:, HALF:]
    c, s, g = cos_f[:, :HALF], sin_f[:, :HALF], sign[:, :HALF]
    edges = jnp.concatenate(
        [
            (s_a[:HALF] + c * s_b[:HALF] - s * s_b[HALF:]) * g,
            (s_a[HALF:] + c * s_b[HALF:] + s * s_b[:HALF]) * g,
        ],
        0,
    ).astype(BF16)
    crossed = lax.dot_general(table[264:272, :HALF], edges, NT, preferred_element_type=F32)
    pad = jnp.zeros((8, HALF), F32)
    first = jnp.concatenate([e_cos + crossed[:, :HALF], pad], 0)
    second = jnp.concatenate([e_sin + crossed[:, HALF:], pad], 0)
    row = lax.broadcasted_iota(jnp.int32, (16, HALF), 0)
    for i in range(4):
        first = jnp.where(row == 4 + i, shifts[0, i].astype(F32), first)
        second = jnp.where(row == 4 + i, shifts[1, i].astype(F32), second)
        w = weights[i].astype(F32)
        if i % 2 == 0:
            first = jnp.where(row == 8 + i // 2, w, first)
        else:
            second = jnp.where(row == 8 + i // 2, w, second)
    out[256:SENT, :HALF] = first.astype(BF16)
    out[256:SENT, HALF:] = second.astype(BF16)


def forward(mask_clip, shifts, weights, table):
    hbm = pl.BlockSpec(memory_space=pltpu.HBM)
    return pl.pallas_call(
        forward_kernel,
        in_specs=[hbm] * 4,
        out_specs=VMEM,
        out_shape=jax.ShapeDtypeStruct((SENT, 256), BF16),
        scratch_shapes=[
            pltpu.SMEM((2, 4), jnp.int32),
            pltpu.SMEM((4,), jnp.int32),
            pltpu.VMEM((2 * TILE, TILE), BF16),
            pltpu.VMEM((272, TILE), BF16),
            pltpu.VMEM((2 * TILE, 256), BF16),
            pltpu.VMEM((TILE, 256), BF16),
            pltpu.SemaphoreType.DMA((3 + len(CHUNKS),)),
        ],
        compiler_params=pltpu.CompilerParams(vmem_limit_bytes=16 * 1024 * 1024),
        cost_estimate=pl.CostEstimate(flops=1_700_000_000, bytes_accessed=5_000_000, transcendentals=0),
        name="forward",
    )(*[pltpu.with_memory_space_constraint(x, pltpu.HBM) for x in (shifts, weights, mask_clip, table)])


def add_kernel(own, one, two, three, out):
    out[...] = (
        own[:SUMMED].astype(F32) + one[:SUMMED].astype(F32)
        + two[:SUMMED].astype(F32) + three[:SUMMED].astype(F32)
    ).astype(BF16)


def add(*args):
    return pl.pallas_call(
        add_kernel,
        in_specs=[VMEM] * 4,
        out_specs=VMEM,
        out_shape=jax.ShapeDtypeStruct((SUMMED, 256), BF16),
        compiler_params=pltpu.CompilerParams(vmem_limit_bytes=4 * 1024 * 1024),
        name="add",
    )(*args)


def pupil_kernel(c0, c1, c2, c3, out):
    f_low = lax.broadcasted_iota(jnp.int32, (HALF, HALF), 0)
    g_low = lax.broadcasted_iota(jnp.int32, (1, HALF), 1)
    f_halves = (f_low.astype(F32), jnp.where(f_low == 0, -HALF, -f_low).astype(F32))
    g_halves = (g_low.astype(F32), jnp.where(g_low == 0, -HALF, -g_low).astype(F32))
    for s in range(16):
        info = (c0, c1, c2, c3)[s // 4][256:SENT].astype(F32)
        i = 4 + s % 4
        a, b = info[i:i + 1, :HALF], info[i:i + 1, HALF:]
        for i, f in enumerate(f_halves):
            room = 4096.0 - (f + a) * (f + a)
            for j, g in enumerate(g_halves):
                reach = (g + b) * (g + b)
                out[s, i * HALF:(i + 1) * HALF, j * HALF:(j + 1) * HALF] = jnp.where(
                    room >= reach, 1.0, 0.0
                ).astype(BF16)


def pupils(*args):
    return pl.pallas_call(
        pupil_kernel,
        in_specs=[VMEM] * 4,
        out_specs=VMEM,
        out_shape=jax.ShapeDtypeStruct((16, 256, 256), BF16),
        compiler_params=pltpu.CompilerParams(vmem_limit_bytes=8 * 1024 * 1024),
        cost_estimate=pl.CostEstimate(flops=10_000_000, bytes_accessed=2_000_000, transcendentals=0),
        name="pupils",
    )(*args)


def inverse_kernel(mine, other, c0, c1, c2, c3, pupil, left, right, spread, sine, out, spec, fields):
    total = mine[:256].astype(F32) + other[:256].astype(F32)
    cc, cs = total[:HALF, :HALF], total[:HALF, HALF:]
    sc, ss = total[HALF:, :HALF], total[HALF:, HALF:]
    edge = mine[256:SUMMED].astype(F32) + other[256:SUMMED].astype(F32)
    rc, rs, xc, xs = (edge[i:i + 1] for i in range(4))
    row_re = (rc[:, :HALF] + rs[:, HALF:], rc[:, :HALF] - rs[:, HALF:])
    row_im = (rs[:, :HALF] - rc[:, HALF:], rs[:, :HALF] + rc[:, HALF:])
    col_re = (xc[:, :HALF] + xs[:, HALF:], xc[:, :HALF] - xs[:, HALF:])
    col_im = (xs[:, :HALF] - xc[:, HALF:], xs[:, :HALF] + xc[:, HALF:])
    first_row = lax.broadcasted_iota(jnp.int32, (HALF, HALF), 0) == 0
    first_lane = lax.broadcasted_iota(jnp.int32, (HALF, HALF), 1) == 0
    quads = {
        (0, 0): (cc - ss, -(sc + cs)),
        (0, 1): (cc + ss, cs - sc),
        (1, 0): (cc + ss, sc - cs),
        (1, 1): (cc - ss, sc + cs),
    }
    for (i, j), parts in quads.items():
        for at, x, row, col in zip((0, 256), parts, (row_re, row_im), (col_re, col_im)):
            if i == 1:
                x = jnp.where(first_row, row[j], x)
            if j == 1:
                x = jnp.where(first_lane, jnp.broadcast_to(col[i], (HALF, HALF)).T, x)
            spec[at + i * HALF:at + (i + 1) * HALF, j * HALF:(j + 1) * HALF] = x.astype(BF16)

    g_low = lax.broadcasted_iota(jnp.int32, (1, HALF), 1)
    g_all = jnp.concatenate([g_low, jnp.where(g_low == 0, -HALF, -g_low)], 1).astype(F32)
    infos = [c[256:SENT].astype(F32) for c in (c0, c1, c2, c3)]
    ends = [jnp.zeros((1, 1), F32)]

    def weight(s):
        i = s % 4
        return infos[s // 4][8 + i // 2:9 + i // 2, (i % 2) * HALF:(i % 2 + 1) * HALF]

    def propagate(s):
        passed = jnp.concatenate([spec[:256] * pupil[s], spec[256:] * pupil[s]], 0)
        k = jnp.dot(left[...], passed, preferred_element_type=F32)
        fields[s * HALF:(s + 1) * HALF, :256] = k[:HALF].astype(BF16)
        fields[s * HALF:(s + 1) * HALF, 256:] = k[HALF:].astype(BF16)
        b = infos[s // 4][4 + s % 4:5 + s % 4, HALF:]
        at = g_all + jnp.concatenate([b, b], 1)
        r, m = k[0:1], k[HALF:HALF + 1]
        pick = lambda x, v: jnp.sum(jnp.where(at == v, x, 0.0), axis=1, keepdims=True)
        z = pick(m, 64.0) * pick(r, -64.0) - pick(r, 64.0) * pick(m, -64.0)
        ends[0] = ends[0] + weight(s)[:, :1] * z

    def power(group):
        k = fields[group * 512:(group + 1) * 512, :]
        e_re = jnp.dot(k, right[0], preferred_element_type=F32)
        e_im = jnp.dot(k, right[1], preferred_element_type=F32)
        p = e_re * e_re + e_im * e_im
        parts = []
        for i in range(4):
            w = weight(group * 4 + i)
            parts.append(p[i * HALF:(i + 1) * HALF] * jnp.concatenate([w, w], 1))
        return (parts[0] + parts[1]) + (parts[2] + parts[3])

    summed = None
    for group in range(4):
        for s in range(4):
            propagate(group * 4 + s)
        if group:
            p = power(group - 1)
            summed = p if summed is None else summed + p
    summed = summed + power(3)
    high = summed.astype(BF16)
    low = (summed - high.astype(F32)).astype(BF16)
    tail = ends[0] * sine[0:1]
    out[...] = (
        jnp.dot(high, spread[0], preferred_element_type=F32)
        + jnp.dot(low, spread[0], preferred_element_type=F32)
        + jnp.dot(high, spread[1], preferred_element_type=F32)
        + tail
    )


def inverse(*args):
    return pl.pallas_call(
        inverse_kernel,
        in_specs=[VMEM] * len(args),
        out_specs=VMEM,
        out_shape=jax.ShapeDtypeStruct((HALF, NI), F32),
        scratch_shapes=[
            pltpu.VMEM((512, 256), BF16),
            pltpu.VMEM((2048, 512), BF16),
        ],
        compiler_params=pltpu.CompilerParams(vmem_limit_bytes=24 * 1024 * 1024),
        cost_estimate=pl.CostEstimate(flops=2_500_000_000, bytes_accessed=3_000_000, transcendentals=0),
        name="inverse",
    )(*args)


def place_rows(left, place):
    freq = jnp.arange(256, dtype=jnp.int32)
    freq = jnp.where(freq < HALF, freq, jnp.where(freq == HALF, -HALF, HALF - freq))
    eighths = freq * place
    cos_q, sin_q = (x.astype(BF16) for x in quarter(jnp.right_shift(eighths, 1)))
    base = jnp.where(jnp.bitwise_and(eighths, 1) == 1, left[1], left[0])
    c, s = base[0] * cos_q - base[1] * sin_q, base[1] * cos_q + base[0] * sin_q
    return jnp.concatenate([jnp.concatenate([c, -s], 1), jnp.concatenate([s, c], 1)], 0)


def ring(x, k):
    return lax.ppermute(x, "src", [(i, (i + k) % 4) for i in range(4)])


def body(mask_clip, source_shifts, source_weights):
    table = forward_tables()
    left, right, spread, sine = inverse_tables()
    place = lax.axis_index("row") * 4 + lax.axis_index("src")
    left_mine = place_rows(jnp.asarray(left, BF16), place)
    own = forward(mask_clip, source_shifts.T, source_weights, jnp.asarray(table, BF16))
    parts = [own] + [ring(own, k) for k in (2, 1, 3)]
    mine = add(*parts)
    other = lax.ppermute(mine, "row", [(0, 1), (1, 0)])
    return inverse(
        mine,
        other,
        *parts,
        pupils(*parts),
        left_mine,
        jnp.asarray(right, BF16),
        jnp.asarray(spread, BF16),
        jnp.asarray(sine, F32),
    )


def solution(mesh):
    placed = (P(("clip", "row"), "src"), P("src", None), P("src"))
    return jax.shard_map(
        body, mesh=mesh, in_specs=placed, out_specs=P(("clip", "row", "src"), None), check_vma=False
    )
```

```python
import jax
import jax.numpy as jnp
import numpy as np
from jax import lax
from jax.experimental import pallas as pl
from jax.experimental.pallas import tpu as pltpu
from jax.sharding import PartitionSpec as P

NM = 4096
NI = 1024
TILE = NM // 4
HALF = 128
CHUNKS = ((0, 512), (512, 1024), (1024, 1536), (1536, 2048))
SENT = 272
SUMMED = 264
COARSE = 256
NT = (((1,), (1,)), ((), ()))
F32 = jnp.float32
BF16 = jnp.bfloat16
VMEM = pl.BlockSpec(memory_space=pltpu.VMEM)


def forward_tables():
    freq = np.arange(HALF)
    pos = np.arange(TILE)
    angle = 2.0 * np.pi * ((freq[:, None] * pos[None, :]) % NM) / NM
    edge = 2.0 * np.pi * ((HALF * pos) % NM) / NM
    table = np.zeros((272, TILE), np.float64)
    table[:HALF] = np.cos(angle)
    table[HALF:256] = np.sin(angle)
    table[256] = np.cos(edge)
    table[257] = np.sin(edge)
    table[266, :HALF] = np.cos(edge[:HALF])
    table[267, :HALF] = np.sin(edge[:HALF])
    return (table / 64).astype(np.float32)


def inverse_tables():
    freq = np.concatenate([np.arange(HALF), -np.arange(HALF)])
    freq[HALF] = -HALF
    rows = np.arange(NI)
    angle = 2.0 * np.pi * ((rows[:, None] * freq[None, :]) % NI) / NI
    left = [np.stack([np.cos(angle[:HALF] + t), np.sin(angle[:HALF] + t)]) / 16 for t in (0.0, np.pi / 4)]
    left = np.stack(left)
    cos_y, sin_y = np.cos(angle[::4]).T / 64, np.sin(angle[::4]).T / 64
    right = np.stack([np.concatenate([cos_y, -sin_y], 0), np.concatenate([sin_y, cos_y], 0)])
    j = np.arange(COARSE)
    harmonic = np.arange(1, HALF)
    columns = np.arange(NI)
    distance = (columns[None, :] - 4 * j[:, None]) % NI
    lags = 2.0 * np.pi * ((np.arange(NI)[:, None] * harmonic[None, :]) % NI) / NI
    wave = (1.0 + 2.0 * np.cos(lags).sum(1) + np.cos(2.0 * np.pi * (np.arange(NI) * HALF % NI) / NI)) / COARSE
    spread = wave[distance]
    high = np.asarray(spread.astype(np.float32).astype(BF16), np.float64)
    spread = np.stack([high, spread - high])
    sine = np.zeros((8, NI), np.float64)
    sine[0] = -2.0 * np.sin(np.pi * (columns % 8) / 4) / 4096
    return tuple(x.astype(np.float32) for x in (left, right, spread, sine))


def quarter(turns):
    q = jnp.bitwise_and(turns, 3)
    cos_q = jnp.where(q == 0, 1.0, jnp.where(q == 2, -1.0, 0.0)).astype(F32)
    sin_q = jnp.where(q == 1, 1.0, jnp.where(q == 3, -1.0, 0.0)).astype(F32)
    return cos_q, sin_q


def forward_kernel(shifts_in, weights_in, mask, table_in, out,
                   shifts, weights, block, table, half_way, folded, sem):
    small_copies = [
        pltpu.make_async_copy(table_in, table, sem.at[0]),
        pltpu.make_async_copy(shifts_in, shifts, sem.at[1]),
        pltpu.make_async_copy(weights_in, weights, sem.at[2]),
    ]
    copies = [
        pltpu.make_async_copy(mask.at[start:stop], block.at[start:stop], sem.at[3 + i])
        for i, (start, stop) in enumerate(CHUNKS)
    ]
    for copy in (small_copies[0], *copies, *small_copies[1:]):
        copy.start()
    row_id = lax.axis_index("row")
    src_id = lax.axis_index("src")
    f_col = lax.broadcasted_iota(jnp.int32, (HALF, 256), 0)
    cos_f, sin_f = quarter(f_col)
    sign, _ = quarter(f_col * 2 * row_id)
    cos_g, sin_g = quarter(lax.broadcasted_iota(jnp.int32, (HALF, HALF), 1) * src_id)

    def join_rows(a, b):
        top = (a[:HALF] + cos_f * b[:HALF] - sin_f * b[HALF:256]) * sign
        low = (a[HALF:256] + cos_f * b[HALF:256] + sin_f * b[:HALF]) * sign
        return top, low

    def turn_columns(x):
        c, s = cos_g[:x.shape[0]], sin_g[:x.shape[0]]
        return c * x[:, :HALF] - s * x[:, HALF:], c * x[:, HALF:] + s * x[:, :HALF]

    small_copies[0].wait()
    sums = []
    for copy, (start, stop) in zip(copies, CHUNKS):
        copy.wait()
        part, at = start // TILE, start % TILE
        half_way[start:stop] = lax.dot_general(
            block[start:stop], table[:256, :], NT, preferred_element_type=F32
        ).astype(BF16)
        for low in range(0, stop - start, 64):
            rows = slice(start + low, start + low + 64)
            tiles = [block[rows, tile * HALF:(tile + 1) * HALF] for tile in range(8)]
            while len(tiles) > 1:
                tiles = [tiles[t] + tiles[t + 1] for t in range(0, len(tiles), 2)]
            folded[at + low:at + low + 64, part * HALF:(part + 1) * HALF] = tiles[0]
        if start == TILE:
            sums.append(jnp.dot(table[:264], half_way[:TILE], preferred_element_type=F32))
    sums.append(jnp.dot(table[:264], half_way[TILE:], preferred_element_type=F32))
    sides = jnp.dot(table[:256, :], folded[...], preferred_element_type=F32)
    for copy in small_copies[1:]:
        copy.wait()
    a, b = sums
    for start, x in zip((0, HALF), join_rows(a, b)):
        x_cos, x_sin = turn_columns(x)
        out[start:start + HALF, :HALF] = x_cos.astype(BF16)
        out[start:start + HALF, HALF:] = x_sin.astype(BF16)
    e_cos, e_sin = turn_columns(a[256:] + b[256:])
    s_a, s_b = sides[:, :HALF], sides[:, HALF:]
    c, s, g = cos_f[:, :HALF], sin_f[:, :HALF], sign[:, :HALF]
    edges = jnp.concatenate(
        [
            (s_a[:HALF] + c * s_b[:HALF] - s * s_b[HALF:]) * g,
            (s_a[HALF:] + c * s_b[HALF:] + s * s_b[:HALF]) * g,
        ],
        0,
    ).astype(BF16)
    crossed = lax.dot_general(table[264:272, :HALF], edges, NT, preferred_element_type=F32)
    pad = jnp.zeros((8, HALF), F32)
    first = jnp.concatenate([e_cos + crossed[:, :HALF], pad], 0)
    second = jnp.concatenate([e_sin + crossed[:, HALF:], pad], 0)
    row = lax.broadcasted_iota(jnp.int32, (16, HALF), 0)
    for i in range(4):
        first = jnp.where(row == 4 + i, shifts[0, i].astype(F32), first)
        second = jnp.where(row == 4 + i, shifts[1, i].astype(F32), second)
        w = weights[i].astype(F32)
        if i % 2 == 0:
            first = jnp.where(row == 8 + i // 2, w, first)
        else:
            second = jnp.where(row == 8 + i // 2, w, second)
    out[256:SENT, :HALF] = first.astype(BF16)
    out[256:SENT, HALF:] = second.astype(BF16)


def forward(mask_clip, shifts, weights, table):
    hbm = pl.BlockSpec(memory_space=pltpu.HBM)
    return pl.pallas_call(
        forward_kernel,
        in_specs=[hbm] * 4,
        out_specs=VMEM,
        out_shape=jax.ShapeDtypeStruct((SENT, 256), BF16),
        scratch_shapes=[
            pltpu.SMEM((2, 4), jnp.int32),
            pltpu.SMEM((4,), jnp.int32),
            pltpu.VMEM((2 * TILE, TILE), BF16),
            pltpu.VMEM((272, TILE), BF16),
            pltpu.VMEM((2 * TILE, 256), BF16),
            pltpu.VMEM((TILE, 256), BF16),
            pltpu.SemaphoreType.DMA((3 + len(CHUNKS),)),
        ],
        compiler_params=pltpu.CompilerParams(vmem_limit_bytes=16 * 1024 * 1024),
        cost_estimate=pl.CostEstimate(flops=1_700_000_000, bytes_accessed=5_000_000, transcendentals=0),
        name="forward",
    )(*[pltpu.with_memory_space_constraint(x, pltpu.HBM) for x in (shifts, weights, mask_clip, table)])


def add_kernel(own, one, two, three, out):
    out[...] = (
        own[:SUMMED].astype(F32) + one[:SUMMED].astype(F32)
        + two[:SUMMED].astype(F32) + three[:SUMMED].astype(F32)
    ).astype(BF16)


def add(*args):
    return pl.pallas_call(
        add_kernel,
        in_specs=[VMEM] * 4,
        out_specs=VMEM,
        out_shape=jax.ShapeDtypeStruct((SUMMED, 256), BF16),
        compiler_params=pltpu.CompilerParams(vmem_limit_bytes=4 * 1024 * 1024),
        name="add",
    )(*args)


def pupil_kernel(c0, c1, c2, c3, right_in, spread_in, out, right, spread, sem):
    copies = [
        pltpu.make_async_copy(right_in, right, sem.at[0]),
        pltpu.make_async_copy(spread_in, spread, sem.at[1]),
    ]
    for copy in copies:
        copy.start()
    f_low = lax.broadcasted_iota(jnp.int32, (HALF, HALF), 0)
    g_low = lax.broadcasted_iota(jnp.int32, (1, HALF), 1)
    f_halves = (f_low.astype(F32), jnp.where(f_low == 0, -HALF, -f_low).astype(F32))
    g_halves = (g_low.astype(F32), jnp.where(g_low == 0, -HALF, -g_low).astype(F32))
    for s in range(16):
        info = (c0, c1, c2, c3)[s // 4][256:SENT].astype(F32)
        i = 4 + s % 4
        a, b = info[i:i + 1, :HALF], info[i:i + 1, HALF:]
        for i, f in enumerate(f_halves):
            room = 4096.0 - (f + a) * (f + a)
            for j, g in enumerate(g_halves):
                reach = (g + b) * (g + b)
                out[s, i * HALF:(i + 1) * HALF, j * HALF:(j + 1) * HALF] = jnp.where(
                    room >= reach, 1.0, 0.0
                ).astype(BF16)
    for copy in copies:
        copy.wait()


def pupils(parts, right, spread):
    tables = [pltpu.with_memory_space_constraint(x, pltpu.HBM) for x in (right, spread)]
    return pl.pallas_call(
        pupil_kernel,
        in_specs=[VMEM] * 4 + [pl.BlockSpec(memory_space=pltpu.HBM)] * 2,
        out_specs=[VMEM] * 3,
        out_shape=[
            jax.ShapeDtypeStruct((16, 256, 256), BF16),
            jax.ShapeDtypeStruct(right.shape, BF16),
            jax.ShapeDtypeStruct(spread.shape, BF16),
        ],
        scratch_shapes=[pltpu.SemaphoreType.DMA((2,))],
        compiler_params=pltpu.CompilerParams(vmem_limit_bytes=8 * 1024 * 1024),
        cost_estimate=pl.CostEstimate(flops=10_000_000, bytes_accessed=4_000_000, transcendentals=0),
        name="pupils",
    )(*parts, *tables)


def inverse_kernel(mine, other, c0, c1, c2, c3, pupil, left, right, spread, sine, out, spec, fields):
    total = mine[:256].astype(F32) + other[:256].astype(F32)
    cc, cs = total[:HALF, :HALF], total[:HALF, HALF:]
    sc, ss = total[HALF:, :HALF], total[HALF:, HALF:]
    edge = mine[256:SUMMED].astype(F32) + other[256:SUMMED].astype(F32)
    rc, rs, xc, xs = (edge[i:i + 1] for i in range(4))
    row_re = (rc[:, :HALF] + rs[:, HALF:], rc[:, :HALF] - rs[:, HALF:])
    row_im = (rs[:, :HALF] - rc[:, HALF:], rs[:, :HALF] + rc[:, HALF:])
    col_re = (xc[:, :HALF] + xs[:, HALF:], xc[:, :HALF] - xs[:, HALF:])
    col_im = (xs[:, :HALF] - xc[:, HALF:], xs[:, :HALF] + xc[:, HALF:])
    first_row = lax.broadcasted_iota(jnp.int32, (HALF, HALF), 0) == 0
    first_lane = lax.broadcasted_iota(jnp.int32, (HALF, HALF), 1) == 0
    quads = {
        (0, 0): (cc - ss, -(sc + cs)),
        (0, 1): (cc + ss, cs - sc),
        (1, 0): (cc + ss, sc - cs),
        (1, 1): (cc - ss, sc + cs),
    }
    for (i, j), parts in quads.items():
        for at, x, row, col in zip((0, 256), parts, (row_re, row_im), (col_re, col_im)):
            if i == 1:
                x = jnp.where(first_row, row[j], x)
            if j == 1:
                x = jnp.where(first_lane, jnp.broadcast_to(col[i], (HALF, HALF)).T, x)
            spec[at + i * HALF:at + (i + 1) * HALF, j * HALF:(j + 1) * HALF] = x.astype(BF16)

    g_low = lax.broadcasted_iota(jnp.int32, (1, HALF), 1)
    g_all = jnp.concatenate([g_low, jnp.where(g_low == 0, -HALF, -g_low)], 1).astype(F32)
    infos = [c[256:SENT].astype(F32) for c in (c0, c1, c2, c3)]
    ends = [jnp.zeros((1, 1), F32)]

    def weight(s):
        i = s % 4
        return infos[s // 4][8 + i // 2:9 + i // 2, (i % 2) * HALF:(i % 2 + 1) * HALF]

    def propagate(s):
        passed = jnp.concatenate([spec[:256] * pupil[s], spec[256:] * pupil[s]], 0)
        k = jnp.dot(left[...], passed, preferred_element_type=F32)
        fields[s * HALF:(s + 1) * HALF, :256] = k[:HALF].astype(BF16)
        fields[s * HALF:(s + 1) * HALF, 256:] = k[HALF:].astype(BF16)
        b = infos[s // 4][4 + s % 4:5 + s % 4, HALF:]
        at = g_all + jnp.concatenate([b, b], 1)
        r, m = k[0:1], k[HALF:HALF + 1]
        pick = lambda x, v: jnp.sum(jnp.where(at == v, x, 0.0), axis=1, keepdims=True)
        z = pick(m, 64.0) * pick(r, -64.0) - pick(r, 64.0) * pick(m, -64.0)
        ends[0] = ends[0] + weight(s)[:, :1] * z

    def power(group):
        k = fields[group * 512:(group + 1) * 512, :]
        e_re = jnp.dot(k, right[0], preferred_element_type=F32)
        e_im = jnp.dot(k, right[1], preferred_element_type=F32)
        p = e_re * e_re + e_im * e_im
        parts = []
        for i in range(4):
            w = weight(group * 4 + i)
            parts.append(p[i * HALF:(i + 1) * HALF] * jnp.concatenate([w, w], 1))
        return (parts[0] + parts[1]) + (parts[2] + parts[3])

    summed = None
    for group in range(4):
        for s in range(4):
            propagate(group * 4 + s)
        if group:
            p = power(group - 1)
            summed = p if summed is None else summed + p
    summed = summed + power(3)
    high = summed.astype(BF16)
    low = (summed - high.astype(F32)).astype(BF16)
    tail = ends[0] * sine[0:1]
    out[...] = (
        jnp.dot(high, spread[0], preferred_element_type=F32)
        + jnp.dot(low, spread[0], preferred_element_type=F32)
        + jnp.dot(high, spread[1], preferred_element_type=F32)
        + tail
    )


def inverse(*args):
    return pl.pallas_call(
        inverse_kernel,
        in_specs=[VMEM] * len(args),
        out_specs=VMEM,
        out_shape=jax.ShapeDtypeStruct((HALF, NI), F32),
        scratch_shapes=[
            pltpu.VMEM((512, 256), BF16),
            pltpu.VMEM((2048, 512), BF16),
        ],
        compiler_params=pltpu.CompilerParams(vmem_limit_bytes=24 * 1024 * 1024),
        cost_estimate=pl.CostEstimate(flops=2_500_000_000, bytes_accessed=3_000_000, transcendentals=0),
        name="inverse",
    )(*args)


def place_rows(left, place):
    freq = jnp.arange(256, dtype=jnp.int32)
    freq = jnp.where(freq < HALF, freq, jnp.where(freq == HALF, -HALF, HALF - freq))
    eighths = freq * place
    cos_q, sin_q = (x.astype(BF16) for x in quarter(jnp.right_shift(eighths, 1)))
    base = jnp.where(jnp.bitwise_and(eighths, 1) == 1, left[1], left[0])
    c, s = base[0] * cos_q - base[1] * sin_q, base[1] * cos_q + base[0] * sin_q
    return jnp.concatenate([jnp.concatenate([c, -s], 1), jnp.concatenate([s, c], 1)], 0)


def ring(x, k):
    return lax.ppermute(x, "src", [(i, (i + k) % 4) for i in range(4)])


def body(mask_clip, source_shifts, source_weights):
    table = forward_tables()
    left, right, spread, sine = inverse_tables()
    place = lax.axis_index("row") * 4 + lax.axis_index("src")
    left_mine = place_rows(jnp.asarray(left, BF16), place)
    own = forward(mask_clip, source_shifts.T, source_weights, jnp.asarray(table, BF16))
    parts = [own] + [ring(own, k) for k in (1, 3, 2)]
    mine = add(*parts)
    other = lax.ppermute(mine, "row", [(0, 1), (1, 0)])
    pupil, right, spread = pupils(parts, jnp.asarray(right, BF16), jnp.asarray(spread, BF16))
    return inverse(mine, other, *parts, pupil, left_mine, right, spread, jnp.asarray(sine, F32))


def solution(mesh):
    placed = (P(("clip", "row"), "src"), P("src", None), P("src"))
    return jax.shard_map(
        body, mesh=mesh, in_specs=placed, out_specs=P(("clip", "row", "src"), None), check_vma=False
    )
```

```python
import jax
import jax.numpy as jnp
import numpy as np
from jax import lax
from jax.experimental import pallas as pl
from jax.experimental.pallas import tpu as pltpu
from jax.sharding import PartitionSpec as P

NM = 4096
NI = 1024
TILE = NM // 4
HALF = 128
CHUNK = 512
QUARTER = 64
SENT = 144
COARSE = 256
NT = (((1,), (1,)), ((), ()))
F32 = jnp.float32
BF16 = jnp.bfloat16
VMEM = pl.BlockSpec(memory_space=pltpu.VMEM)


def forward_tables():
    freq = np.arange(HALF)
    pos = np.arange(TILE)
    angle = 2.0 * np.pi * ((freq[:, None] * pos[None, :]) % NM) / NM
    edge = 2.0 * np.pi * ((HALF * pos) % NM) / NM
    table = np.zeros((272, TILE), np.float64)
    table[:HALF] = np.cos(angle)
    table[HALF:256] = np.sin(angle)
    table[256] = np.cos(edge)
    table[257] = np.sin(edge)
    table[266, :HALF] = np.cos(edge[:HALF])
    table[267, :HALF] = np.sin(edge[:HALF])
    return (table / 64).astype(np.float32)


def inverse_tables():
    freq = np.concatenate([np.arange(HALF), -np.arange(HALF)])
    freq[HALF] = -HALF
    rows = np.arange(NI)
    angle = 2.0 * np.pi * ((rows[:, None] * freq[None, :]) % NI) / NI
    left = [np.stack([np.cos(angle[:HALF] + t), np.sin(angle[:HALF] + t)]) / 16 for t in (0.0, np.pi / 4)]
    left = np.stack(left)
    cos_y, sin_y = np.cos(angle[::4]).T / 64, np.sin(angle[::4]).T / 64
    right = np.stack([np.concatenate([cos_y, -sin_y], 0), np.concatenate([sin_y, cos_y], 0)])
    j = np.arange(COARSE)
    harmonic = np.arange(1, HALF)
    columns = np.arange(NI)
    distance = (columns[None, :] - 4 * j[:, None]) % NI
    lags = 2.0 * np.pi * ((np.arange(NI)[:, None] * harmonic[None, :]) % NI) / NI
    wave = (1.0 + 2.0 * np.cos(lags).sum(1) + np.cos(2.0 * np.pi * (np.arange(NI) * HALF % NI) / NI)) / COARSE
    spread = wave[distance]
    high = np.asarray(spread.astype(np.float32).astype(BF16), np.float64)
    spread = np.stack([high, spread - high])
    sine = np.zeros((8, NI), np.float64)
    sine[0] = -2.0 * np.sin(np.pi * (columns % 8) / 4) / 4096
    return tuple(x.astype(np.float32) for x in (left, right, spread, sine))


def quarter(turns):
    q = jnp.bitwise_and(turns, 3)
    cos_q = jnp.where(q == 0, 1.0, jnp.where(q == 2, -1.0, 0.0)).astype(F32)
    sin_q = jnp.where(q == 1, 1.0, jnp.where(q == 3, -1.0, 0.0)).astype(F32)
    return cos_q, sin_q


def forward_kernel(shifts_in, weights_in, mask, table_in, keep, give,
                   shifts, weights, block, table, half_way, folded, whole, sem):
    small_copies = [
        pltpu.make_async_copy(table_in, table, sem.at[0]),
        pltpu.make_async_copy(shifts_in, shifts, sem.at[1]),
        pltpu.make_async_copy(weights_in, weights, sem.at[2]),
    ]
    copies = [
        pltpu.make_async_copy(
            mask.at[i * CHUNK:(i + 1) * CHUNK], block.at[i * CHUNK:(i + 1) * CHUNK], sem.at[3 + i]
        )
        for i in range(4)
    ]
    for copy in (small_copies[0], *copies, *small_copies[1:]):
        copy.start()
    row_id = lax.axis_index("row")
    src_id = lax.axis_index("src")
    f_col = lax.broadcasted_iota(jnp.int32, (HALF, 256), 0)
    cos_f, sin_f = quarter(f_col)
    sign, _ = quarter(f_col * 2 * row_id)
    cos_g, sin_g = quarter(lax.broadcasted_iota(jnp.int32, (HALF, HALF), 1) * src_id)

    def join_rows(a, b):
        top = (a[:HALF] + cos_f * b[:HALF] - sin_f * b[HALF:256]) * sign
        low = (a[HALF:256] + cos_f * b[HALF:256] + sin_f * b[:HALF]) * sign
        return top, low

    def turn_columns(x):
        c, s = cos_g[:x.shape[0]], sin_g[:x.shape[0]]
        return c * x[:, :HALF] - s * x[:, HALF:], c * x[:, HALF:] + s * x[:, :HALF]

    small_copies[0].wait()

    @pl.loop(0, 4)
    def _(i):
        rows = pl.ds(pl.multiple_of(i * CHUNK, CHUNK), CHUNK)
        pltpu.make_async_copy(mask.at[rows], block.at[rows], sem.at[3 + i]).wait()
        half_way[rows] = lax.dot_general(
            block[rows], table[:256, :], NT, preferred_element_type=F32
        ).astype(BF16)
        lanes = pl.ds(pl.multiple_of((i // 2) * HALF, HALF), HALF)
        for low in range(0, CHUNK, 64):
            strip = pl.ds(pl.multiple_of(i * CHUNK + low, 64), 64)
            tiles = [block[strip, tile * HALF:(tile + 1) * HALF] for tile in range(8)]
            while len(tiles) > 1:
                tiles = [tiles[t] + tiles[t + 1] for t in range(0, len(tiles), 2)]
            folded[pl.ds(pl.multiple_of(lax.rem(i, 2) * CHUNK + low, 64), 64), lanes] = tiles[0]

    sums = [
        jnp.dot(table[:264], half_way[h * TILE:(h + 1) * TILE], preferred_element_type=F32)
        for h in range(2)
    ]
    sides = jnp.dot(table[:256, :], folded[...], preferred_element_type=F32)
    for copy in small_copies[1:]:
        copy.wait()
    a, b = sums
    for start, x in zip((0, HALF), join_rows(a, b)):
        x_cos, x_sin = turn_columns(x)
        whole[start:start + HALF, :HALF] = x_cos
        whole[start:start + HALF, HALF:] = x_sin
    e_cos, e_sin = turn_columns(a[256:] + b[256:])
    s_a, s_b = sides[:, :HALF], sides[:, HALF:]
    c, s, g = cos_f[:, :HALF], sin_f[:, :HALF], sign[:, :HALF]
    edges = jnp.concatenate(
        [
            (s_a[:HALF] + c * s_b[:HALF] - s * s_b[HALF:]) * g,
            (s_a[HALF:] + c * s_b[HALF:] + s * s_b[:HALF]) * g,
        ],
        0,
    ).astype(BF16)
    crossed = lax.dot_general(table[264:272, :HALF], edges, NT, preferred_element_type=F32)
    edges = jnp.concatenate([e_cos + crossed[:, :HALF], e_sin + crossed[:, HALF:]], 1)
    row = lax.broadcasted_iota(jnp.int32, (16, HALF), 0)
    first = jnp.zeros((16, HALF), F32)
    second = jnp.zeros((16, HALF), F32)
    for i in range(4):
        first = jnp.where(row == 2 + i, shifts[0, i].astype(F32), first)
        second = jnp.where(row == 2 + i, shifts[1, i].astype(F32), second)
        w = weights[i].astype(F32)
        if i % 2 == 0:
            first = jnp.where(row == 6 + i // 2, w, first)
        else:
            second = jnp.where(row == 6 + i // 2, w, second)
    sources = jnp.concatenate([first, second], 1)
    row = lax.broadcasted_iota(jnp.int32, (16, 256), 0)
    for out, odd in ((keep, lax.rem(src_id, 2)), (give, lax.rem(src_id + 1, 2))):
        at = pl.multiple_of(odd * QUARTER, QUARTER)
        out[:QUARTER] = whole[pl.ds(at, QUARTER)].astype(BF16)
        out[QUARTER:HALF] = whole[pl.ds(HALF + at, QUARTER)].astype(BF16)
        lines = [jnp.where(odd == 1, edges[2 + i:3 + i], edges[i:i + 1]) for i in range(2)]
        out[HALF:SENT] = jnp.where(
            row == 0, lines[0], jnp.where(row == 1, lines[1], sources)
        ).astype(BF16)


def forward(mask_clip, shifts, weights, table):
    hbm = pl.BlockSpec(memory_space=pltpu.HBM)
    return pl.pallas_call(
        forward_kernel,
        in_specs=[hbm] * 4,
        out_specs=[VMEM] * 2,
        out_shape=[jax.ShapeDtypeStruct((SENT, 256), BF16)] * 2,
        scratch_shapes=[
            pltpu.SMEM((2, 4), jnp.int32),
            pltpu.SMEM((4,), jnp.int32),
            pltpu.VMEM((2 * TILE, TILE), BF16),
            pltpu.VMEM((272, TILE), BF16),
            pltpu.VMEM((2 * TILE, 256), BF16),
            pltpu.VMEM((TILE, 256), BF16),
            pltpu.VMEM((256, 256), F32),
            pltpu.SemaphoreType.DMA((7,)),
        ],
        compiler_params=pltpu.CompilerParams(vmem_limit_bytes=16 * 1024 * 1024),
        cost_estimate=pl.CostEstimate(flops=1_700_000_000, bytes_accessed=5_000_000, transcendentals=0),
        name="forward",
    )(*[pltpu.with_memory_space_constraint(x, pltpu.HBM) for x in (shifts, weights, mask_clip, table)])


def add_kernel(own, one, two, three, out):
    out[...] = (
        own[...].astype(F32) + one[...].astype(F32) + two[...].astype(F32) + three[...].astype(F32)
    ).astype(BF16)


def finish_kernel(mine, other, out):
    total = mine[...].astype(F32) + other[...].astype(F32)
    cc, cs = total[:QUARTER, :HALF], total[:QUARTER, HALF:]
    sc, ss = total[QUARTER:HALF, :HALF], total[QUARTER:HALF, HALF:]
    out[:QUARTER, :HALF] = (cc - ss).astype(BF16)
    out[:QUARTER, HALF:] = (cc + ss).astype(BF16)
    out[QUARTER:HALF, :HALF] = (-(sc + cs)).astype(BF16)
    out[QUARTER:HALF, HALF:] = (cs - sc).astype(BF16)
    out[HALF:] = total[HALF:].astype(BF16)


def small(kernel, name, *args):
    return pl.pallas_call(
        kernel,
        in_specs=[VMEM] * len(args),
        out_specs=VMEM,
        out_shape=jax.ShapeDtypeStruct((SENT, 256), BF16),
        compiler_params=pltpu.CompilerParams(vmem_limit_bytes=4 * 1024 * 1024),
        name=name,
    )(*args)


def pupil_kernel(c0, c1, c2, c3, right_in, spread_in, out, right, spread, sem):
    copies = [
        pltpu.make_async_copy(right_in, right, sem.at[0]),
        pltpu.make_async_copy(spread_in, spread, sem.at[1]),
    ]
    for copy in copies:
        copy.start()
    f_low = lax.broadcasted_iota(jnp.int32, (HALF, HALF), 0)
    g_low = lax.broadcasted_iota(jnp.int32, (1, HALF), 1)
    f_halves = (f_low.astype(F32), jnp.where(f_low == 0, -HALF, -f_low).astype(F32))
    g_halves = (g_low.astype(F32), jnp.where(g_low == 0, -HALF, -g_low).astype(F32))
    for s in range(16):
        info = (c0, c1, c2, c3)[s // 4][HALF:SENT].astype(F32)
        i = 2 + s % 4
        a, b = info[i:i + 1, :HALF], info[i:i + 1, HALF:]
        for i, f in enumerate(f_halves):
            room = 4096.0 - (f + a) * (f + a)
            for j, g in enumerate(g_halves):
                reach = (g + b) * (g + b)
                out[s, i * HALF:(i + 1) * HALF, j * HALF:(j + 1) * HALF] = jnp.where(
                    room >= reach, 1.0, 0.0
                ).astype(BF16)
    for copy in copies:
        copy.wait()


def pupils(parts, right, spread):
    tables = [pltpu.with_memory_space_constraint(x, pltpu.HBM) for x in (right, spread)]
    return pl.pallas_call(
        pupil_kernel,
        in_specs=[VMEM] * 4 + [pl.BlockSpec(memory_space=pltpu.HBM)] * 2,
        out_specs=[VMEM] * 3,
        out_shape=[
            jax.ShapeDtypeStruct((16, 256, 256), BF16),
            jax.ShapeDtypeStruct(right.shape, BF16),
            jax.ShapeDtypeStruct(spread.shape, BF16),
        ],
        scratch_shapes=[pltpu.SemaphoreType.DMA((2,))],
        compiler_params=pltpu.CompilerParams(vmem_limit_bytes=8 * 1024 * 1024),
        cost_estimate=pl.CostEstimate(flops=10_000_000, bytes_accessed=4_000_000, transcendentals=0),
        name="pupils",
    )(*parts, *tables)


def inverse_kernel(mine, other, c0, c1, c2, c3, pupil, left, right, spread, sine, out,
                   spec, edge, fields):
    src_id = lax.axis_index("src")
    for chunk, odd in ((mine, lax.rem(src_id, 2)), (other, lax.rem(src_id + 1, 2))):
        at = pl.multiple_of(odd * QUARTER, QUARTER)
        re, im = chunk[:QUARTER], chunk[QUARTER:HALF]
        spec[pl.ds(at, QUARTER)] = re
        spec[pl.ds(256 + at, QUARTER)] = im
        spec[pl.ds(HALF + at, QUARTER), :HALF] = re[:, HALF:]
        spec[pl.ds(HALF + at, QUARTER), HALF:] = re[:, :HALF]
        spec[pl.ds(384 + at, QUARTER), :HALF] = -im[:, HALF:]
        spec[pl.ds(384 + at, QUARTER), HALF:] = -im[:, :HALF]
        lines = chunk[HALF:SENT].astype(F32)
        edge[pl.ds(odd * 2, 1)] = lines[0:1]
        edge[pl.ds(odd * 2 + 1, 1)] = lines[1:2]
    rc, rs, xc, xs = (edge[i:i + 1] for i in range(4))
    row_re = jnp.concatenate([rc[:, :HALF] + rs[:, HALF:], rc[:, :HALF] - rs[:, HALF:]], 1)
    row_im = jnp.concatenate([rs[:, :HALF] - rc[:, HALF:], rs[:, :HALF] + rc[:, HALF:]], 1)
    col_re = jnp.concatenate([xc[:, :HALF] + xs[:, HALF:], xc[:, :HALF] - xs[:, HALF:]], 1)
    col_im = jnp.concatenate([xs[:, :HALF] - xc[:, HALF:], xs[:, :HALF] + xc[:, HALF:]], 1)
    top = lax.broadcasted_iota(jnp.int32, (16, 256), 0) == 0
    first_lane = lax.broadcasted_iota(jnp.int32, (HALF, HALF), 1) == 0
    for at, row, col in ((0, row_re, col_re), (256, row_im, col_im)):
        low = slice(at + HALF, at + HALF + 16)
        spec[low] = jnp.where(top, row, spec[low].astype(F32)).astype(BF16)
        for i in range(2):
            rows = slice(at + i * HALF, at + (i + 1) * HALF)
            stood = jnp.broadcast_to(col[:, i * HALF:(i + 1) * HALF], (HALF, HALF)).T
            spec[rows, HALF:] = jnp.where(first_lane, stood, spec[rows, HALF:].astype(F32)).astype(BF16)

    g_low = lax.broadcasted_iota(jnp.int32, (1, HALF), 1)
    g_all = jnp.concatenate([g_low, jnp.where(g_low == 0, -HALF, -g_low)], 1).astype(F32)
    infos = [c[HALF:SENT].astype(F32) for c in (c0, c1, c2, c3)]
    ends = [jnp.zeros((1, 1), F32)]

    def weight(s):
        i = s % 4
        return infos[s // 4][6 + i // 2:7 + i // 2, (i % 2) * HALF:(i % 2 + 1) * HALF]

    def propagate(s):
        passed = jnp.concatenate([spec[:256] * pupil[s], spec[256:] * pupil[s]], 0)
        k = jnp.dot(left[...], passed, preferred_element_type=F32)
        fields[s * HALF:(s + 1) * HALF, :256] = k[:HALF].astype(BF16)
        fields[s * HALF:(s + 1) * HALF, 256:] = k[HALF:].astype(BF16)
        b = infos[s // 4][2 + s % 4:3 + s % 4, HALF:]
        at = g_all + jnp.concatenate([b, b], 1)
        r, m = k[0:1], k[HALF:HALF + 1]
        pick = lambda x, v: jnp.sum(jnp.where(at == v, x, 0.0), axis=1, keepdims=True)
        z = pick(m, 64.0) * pick(r, -64.0) - pick(r, 64.0) * pick(m, -64.0)
        ends[0] = ends[0] + weight(s)[:, :1] * z

    def power(group):
        k = fields[group * 512:(group + 1) * 512, :]
        e_re = jnp.dot(k, right[0], preferred_element_type=F32)
        e_im = jnp.dot(k, right[1], preferred_element_type=F32)
        p = e_re * e_re + e_im * e_im
        parts = []
        for i in range(4):
            w = weight(group * 4 + i)
            parts.append(p[i * HALF:(i + 1) * HALF] * jnp.concatenate([w, w], 1))
        return (parts[0] + parts[1]) + (parts[2] + parts[3])

    summed = None
    for group in range(4):
        for s in range(4):
            propagate(group * 4 + s)
        if group:
            p = power(group - 1)
            summed = p if summed is None else summed + p
    summed = summed + power(3)
    high = summed.astype(BF16)
    low = (summed - high.astype(F32)).astype(BF16)
    tail = ends[0] * sine[0:1]
    out[...] = (
        jnp.dot(high, spread[0], preferred_element_type=F32)
        + jnp.dot(low, spread[0], preferred_element_type=F32)
        + jnp.dot(high, spread[1], preferred_element_type=F32)
        + tail
    )


def inverse(*args):
    return pl.pallas_call(
        inverse_kernel,
        in_specs=[VMEM] * len(args),
        out_specs=VMEM,
        out_shape=jax.ShapeDtypeStruct((HALF, NI), F32),
        scratch_shapes=[
            pltpu.VMEM((512, 256), BF16),
            pltpu.VMEM((8, 256), F32),
            pltpu.VMEM((2048, 512), BF16),
        ],
        compiler_params=pltpu.CompilerParams(vmem_limit_bytes=24 * 1024 * 1024),
        cost_estimate=pl.CostEstimate(flops=2_500_000_000, bytes_accessed=3_000_000, transcendentals=0),
        name="inverse",
    )(*args)


def place_rows(left, place):
    freq = jnp.arange(256, dtype=jnp.int32)
    freq = jnp.where(freq < HALF, freq, jnp.where(freq == HALF, -HALF, HALF - freq))
    eighths = freq * place
    cos_q, sin_q = (x.astype(BF16) for x in quarter(jnp.right_shift(eighths, 1)))
    base = jnp.where(jnp.bitwise_and(eighths, 1) == 1, left[1], left[0])
    c, s = base[0] * cos_q - base[1] * sin_q, base[1] * cos_q + base[0] * sin_q
    return jnp.concatenate([jnp.concatenate([c, -s], 1), jnp.concatenate([s, c], 1)], 0)


def ring(x, k):
    return lax.ppermute(x, "src", [(i, (i + k) % 4) for i in range(4)])


def body(mask_clip, source_shifts, source_weights):
    table = forward_tables()
    left, right, spread, sine = inverse_tables()
    place = lax.axis_index("row") * 4 + lax.axis_index("src")
    left_mine = place_rows(jnp.asarray(left, BF16), place)
    keep, give = forward(mask_clip, source_shifts.T, source_weights, jnp.asarray(table, BF16))
    parts = [keep, ring(give, 1), ring(give, 3), ring(keep, 2)]
    summed = small(add_kernel, "add", *parts)
    mine = small(finish_kernel, "finish", summed, lax.ppermute(summed, "row", [(0, 1), (1, 0)]))
    other = lax.ppermute(mine, "src", [(0, 1), (1, 0), (2, 3), (3, 2)])
    pupil, right, spread = pupils(parts, jnp.asarray(right, BF16), jnp.asarray(spread, BF16))
    return inverse(mine, other, *parts, pupil, left_mine, right, spread, jnp.asarray(sine, F32))


def solution(mesh):
    placed = (P(("clip", "row"), "src"), P("src", None), P("src"))
    return jax.shard_map(
        body, mesh=mesh, in_specs=placed, out_specs=P(("clip", "row", "src"), None), check_vma=False
    )
```

```python
import jax
import jax.numpy as jnp
import numpy as np
from jax import lax
from jax.experimental import pallas as pl
from jax.experimental.pallas import tpu as pltpu
from jax.sharding import PartitionSpec as P

NM = 4096
NI = 1024
TILE = NM // 4
HALF = 128
CHUNK = 512
QUARTER = 64
SENT = 136
COARSE = 256
NT = (((1,), (1,)), ((), ()))
F32 = jnp.float32
BF16 = jnp.bfloat16
VMEM = pl.BlockSpec(memory_space=pltpu.VMEM)


def forward_tables():
    freq = np.arange(HALF)
    pos = np.arange(TILE)
    angle = 2.0 * np.pi * ((freq[:, None] * pos[None, :]) % NM) / NM
    edge = 2.0 * np.pi * ((HALF * pos) % NM) / NM
    table = np.zeros((272, TILE), np.float64)
    table[:HALF] = np.cos(angle)
    table[HALF:256] = np.sin(angle)
    table[256] = np.cos(edge)
    table[257] = np.sin(edge)
    table[266, :HALF] = np.cos(edge[:HALF])
    table[267, :HALF] = np.sin(edge[:HALF])
    return (table / 64).astype(np.float32)


def inverse_tables():
    freq = np.concatenate([np.arange(HALF), -np.arange(HALF)])
    freq[HALF] = -HALF
    rows = np.arange(NI)
    angle = 2.0 * np.pi * ((rows[:, None] * freq[None, :]) % NI) / NI
    left = [np.stack([np.cos(angle[:HALF] + t), np.sin(angle[:HALF] + t)]) / 16 for t in (0.0, np.pi / 4)]
    left = np.stack(left)
    cos_y, sin_y = np.cos(angle[::4]).T / 64, np.sin(angle[::4]).T / 64
    right = np.stack([np.concatenate([cos_y, -sin_y], 0), np.concatenate([sin_y, cos_y], 0)])
    j = np.arange(COARSE)
    harmonic = np.arange(1, HALF)
    columns = np.arange(NI)
    distance = (columns[None, :] - 4 * j[:, None]) % NI
    lags = 2.0 * np.pi * ((np.arange(NI)[:, None] * harmonic[None, :]) % NI) / NI
    wave = (1.0 + 2.0 * np.cos(lags).sum(1) + np.cos(2.0 * np.pi * (np.arange(NI) * HALF % NI) / NI)) / COARSE
    spread = wave[distance]
    high = np.asarray(spread.astype(np.float32).astype(BF16), np.float64)
    spread = np.stack([high, spread - high])
    sine = np.zeros((8, NI), np.float64)
    sine[0] = -2.0 * np.sin(np.pi * (columns % 8) / 4) / 4096
    return tuple(x.astype(np.float32) for x in (left, right, spread, sine))


def quarter(turns):
    q = jnp.bitwise_and(turns, 3)
    cos_q = jnp.where(q == 0, 1.0, jnp.where(q == 2, -1.0, 0.0)).astype(F32)
    sin_q = jnp.where(q == 1, 1.0, jnp.where(q == 3, -1.0, 0.0)).astype(F32)
    return cos_q, sin_q


def forward_kernel(shifts_in, weights_in, mask, table_in, far, after, before, keep,
                   shifts, weights, block, table, half_way, folded, whole, sem):
    small_copies = [
        pltpu.make_async_copy(table_in, table, sem.at[0]),
        pltpu.make_async_copy(shifts_in, shifts, sem.at[1]),
        pltpu.make_async_copy(weights_in, weights, sem.at[2]),
    ]
    copies = [
        pltpu.make_async_copy(
            mask.at[i * CHUNK:(i + 1) * CHUNK], block.at[i * CHUNK:(i + 1) * CHUNK], sem.at[3 + i]
        )
        for i in range(4)
    ]
    for copy in (small_copies[0], *copies, *small_copies[1:]):
        copy.start()
    row_id = lax.axis_index("row")
    src_id = lax.axis_index("src")
    f_col = lax.broadcasted_iota(jnp.int32, (HALF, 256), 0)
    cos_f, sin_f = quarter(f_col)
    sign, _ = quarter(f_col * 2 * row_id)
    cos_g, sin_g = quarter(lax.broadcasted_iota(jnp.int32, (HALF, HALF), 1) * src_id)

    def join_rows(a, b):
        top = (a[:HALF] + cos_f * b[:HALF] - sin_f * b[HALF:256]) * sign
        low = (a[HALF:256] + cos_f * b[HALF:256] + sin_f * b[:HALF]) * sign
        return top, low

    def turn_columns(x):
        c, s = cos_g[:x.shape[0]], sin_g[:x.shape[0]]
        return c * x[:, :HALF] - s * x[:, HALF:], c * x[:, HALF:] + s * x[:, :HALF]

    small_copies[0].wait()

    @pl.loop(0, 4)
    def _(i):
        rows = pl.ds(pl.multiple_of(i * CHUNK, CHUNK), CHUNK)
        pltpu.make_async_copy(mask.at[rows], block.at[rows], sem.at[3 + i]).wait()
        half_way[rows] = lax.dot_general(
            block[rows], table[:256, :], NT, preferred_element_type=F32
        ).astype(BF16)
        lanes = pl.ds(pl.multiple_of((i // 2) * HALF, HALF), HALF)
        for low in range(0, CHUNK, 64):
            strip = pl.ds(pl.multiple_of(i * CHUNK + low, 64), 64)
            tiles = [block[strip, tile * HALF:(tile + 1) * HALF] for tile in range(8)]
            while len(tiles) > 1:
                tiles = [tiles[t] + tiles[t + 1] for t in range(0, len(tiles), 2)]
            folded[pl.ds(pl.multiple_of(lax.rem(i, 2) * CHUNK + low, 64), 64), lanes] = tiles[0]

    sums = [
        jnp.dot(table[:264], half_way[h * TILE:(h + 1) * TILE], preferred_element_type=F32)
        for h in range(2)
    ]
    sides = jnp.dot(table[:256, :], folded[...], preferred_element_type=F32)
    for copy in small_copies[1:]:
        copy.wait()
    a, b = sums
    for start, x in zip((0, HALF), join_rows(a, b)):
        x_cos, x_sin = turn_columns(x)
        whole[start:start + HALF, :HALF] = x_cos
        whole[start:start + HALF, HALF:] = x_sin
    e_cos, e_sin = turn_columns(a[256:] + b[256:])
    s_a, s_b = sides[:, :HALF], sides[:, HALF:]
    c, s, g = cos_f[:, :HALF], sin_f[:, :HALF], sign[:, :HALF]
    edges = jnp.concatenate(
        [
            (s_a[:HALF] + c * s_b[:HALF] - s * s_b[HALF:]) * g,
            (s_a[HALF:] + c * s_b[HALF:] + s * s_b[:HALF]) * g,
        ],
        0,
    ).astype(BF16)
    crossed = lax.dot_general(table[264:272, :HALF], edges, NT, preferred_element_type=F32)
    edges = jnp.concatenate([e_cos + crossed[:, :HALF], e_sin + crossed[:, HALF:]], 1)
    row = lax.broadcasted_iota(jnp.int32, (8, HALF), 0)
    first = jnp.zeros((8, HALF), F32)
    second = jnp.zeros((8, HALF), F32)
    for i in range(4):
        first = jnp.where(row == 2 + i, shifts[0, i].astype(F32), first)
        second = jnp.where(row == 2 + i, shifts[1, i].astype(F32), second)
        w = weights[i].astype(F32)
        if i % 2 == 0:
            first = jnp.where(row == 6 + i // 2, w, first)
        else:
            second = jnp.where(row == 6 + i // 2, w, second)
    sources = jnp.concatenate([first, second], 1)
    row = lax.broadcasted_iota(jnp.int32, (8, 256), 0)
    for outs, odd in (((far, keep), lax.rem(src_id, 2)), ((after, before), lax.rem(src_id + 1, 2))):
        at = pl.multiple_of(odd * QUARTER, QUARTER)
        lines = [jnp.where(odd == 1, edges[2 + i:3 + i], edges[i:i + 1]) for i in range(2)]
        rows = jnp.where(row == 0, lines[0], jnp.where(row == 1, lines[1], sources)).astype(BF16)
        cos_rows = whole[pl.ds(at, QUARTER)].astype(BF16)
        sin_rows = whole[pl.ds(HALF + at, QUARTER)].astype(BF16)
        for out in outs:
            out[:QUARTER] = cos_rows
            out[QUARTER:HALF] = sin_rows
            out[HALF:SENT] = rows


def forward(mask_clip, shifts, weights, table):
    hbm = pl.BlockSpec(memory_space=pltpu.HBM)
    return pl.pallas_call(
        forward_kernel,
        in_specs=[hbm] * 4,
        out_specs=[VMEM] * 4,
        out_shape=[jax.ShapeDtypeStruct((SENT, 256), BF16)] * 4,
        scratch_shapes=[
            pltpu.SMEM((2, 4), jnp.int32),
            pltpu.SMEM((4,), jnp.int32),
            pltpu.VMEM((2 * TILE, TILE), BF16),
            pltpu.VMEM((272, TILE), BF16),
            pltpu.VMEM((2 * TILE, 256), BF16),
            pltpu.VMEM((TILE, 256), BF16),
            pltpu.VMEM((256, 256), F32),
            pltpu.SemaphoreType.DMA((7,)),
        ],
        compiler_params=pltpu.CompilerParams(vmem_limit_bytes=16 * 1024 * 1024),
        cost_estimate=pl.CostEstimate(flops=1_700_000_000, bytes_accessed=5_000_000, transcendentals=0),
        name="forward",
    )(*[pltpu.with_memory_space_constraint(x, pltpu.HBM) for x in (shifts, weights, mask_clip, table)])


def add_kernel(own, one, two, three, out):
    out[...] = (
        own[...].astype(F32) + one[...].astype(F32) + two[...].astype(F32) + three[...].astype(F32)
    ).astype(BF16)


def finish_kernel(mine, other, out):
    total = mine[...].astype(F32) + other[...].astype(F32)
    cc, cs = total[:QUARTER, :HALF], total[:QUARTER, HALF:]
    sc, ss = total[QUARTER:HALF, :HALF], total[QUARTER:HALF, HALF:]
    out[:QUARTER, :HALF] = (cc - ss).astype(BF16)
    out[:QUARTER, HALF:] = (cc + ss).astype(BF16)
    out[QUARTER:HALF, :HALF] = (-(sc + cs)).astype(BF16)
    out[QUARTER:HALF, HALF:] = (cs - sc).astype(BF16)
    out[HALF:] = total[HALF:].astype(BF16)


def small(kernel, name, *args):
    return pl.pallas_call(
        kernel,
        in_specs=[VMEM] * len(args),
        out_specs=VMEM,
        out_shape=jax.ShapeDtypeStruct((SENT, 256), BF16),
        compiler_params=pltpu.CompilerParams(vmem_limit_bytes=4 * 1024 * 1024),
        name=name,
    )(*args)


def pupil_kernel(c0, c1, c2, c3, right_in, spread_in, out, right, spread, sem):
    copies = [
        pltpu.make_async_copy(right_in, right, sem.at[0]),
        pltpu.make_async_copy(spread_in, spread, sem.at[1]),
    ]
    for copy in copies:
        copy.start()
    f_low = lax.broadcasted_iota(jnp.int32, (HALF, HALF), 0)
    g_low = lax.broadcasted_iota(jnp.int32, (1, HALF), 1)
    f_halves = (f_low.astype(F32), jnp.where(f_low == 0, -HALF, -f_low).astype(F32))
    g_halves = (g_low.astype(F32), jnp.where(g_low == 0, -HALF, -g_low).astype(F32))
    for s in range(16):
        info = (c0, c1, c2, c3)[s // 4][HALF:SENT].astype(F32)
        i = 2 + s % 4
        a, b = info[i:i + 1, :HALF], info[i:i + 1, HALF:]
        for i, f in enumerate(f_halves):
            room = 4096.0 - (f + a) * (f + a)
            for j, g in enumerate(g_halves):
                reach = (g + b) * (g + b)
                out[s, i * HALF:(i + 1) * HALF, j * HALF:(j + 1) * HALF] = jnp.where(
                    room >= reach, 1.0, 0.0
                ).astype(BF16)
    for copy in copies:
        copy.wait()


def pupils(parts, right, spread):
    tables = [pltpu.with_memory_space_constraint(x, pltpu.HBM) for x in (right, spread)]
    return pl.pallas_call(
        pupil_kernel,
        in_specs=[VMEM] * 4 + [pl.BlockSpec(memory_space=pltpu.HBM)] * 2,
        out_specs=[VMEM] * 3,
        out_shape=[
            jax.ShapeDtypeStruct((16, 256, 256), BF16),
            jax.ShapeDtypeStruct(right.shape, BF16),
            jax.ShapeDtypeStruct(spread.shape, BF16),
        ],
        scratch_shapes=[pltpu.SemaphoreType.DMA((2,))],
        compiler_params=pltpu.CompilerParams(vmem_limit_bytes=8 * 1024 * 1024),
        cost_estimate=pl.CostEstimate(flops=10_000_000, bytes_accessed=4_000_000, transcendentals=0),
        name="pupils",
    )(*parts, *tables)


def inverse_kernel(mine, other, c0, c1, c2, c3, pupil, left, right, spread, sine, out,
                   spec, edge, fields, image, sem):
    src_id = lax.axis_index("src")
    for chunk, odd in ((mine, lax.rem(src_id, 2)), (other, lax.rem(src_id + 1, 2))):
        at = pl.multiple_of(odd * QUARTER, QUARTER)
        re, im = chunk[:QUARTER], chunk[QUARTER:HALF]
        spec[pl.ds(at, QUARTER)] = re
        spec[pl.ds(256 + at, QUARTER)] = im
        spec[pl.ds(HALF + at, QUARTER), :HALF] = re[:, HALF:]
        spec[pl.ds(HALF + at, QUARTER), HALF:] = re[:, :HALF]
        spec[pl.ds(384 + at, QUARTER), :HALF] = -im[:, HALF:]
        spec[pl.ds(384 + at, QUARTER), HALF:] = -im[:, :HALF]
        lines = chunk[HALF:SENT].astype(F32)
        edge[pl.ds(odd * 2, 1)] = lines[0:1]
        edge[pl.ds(odd * 2 + 1, 1)] = lines[1:2]
    rc, rs, xc, xs = (edge[i:i + 1] for i in range(4))
    row_re = jnp.concatenate([rc[:, :HALF] + rs[:, HALF:], rc[:, :HALF] - rs[:, HALF:]], 1)
    row_im = jnp.concatenate([rs[:, :HALF] - rc[:, HALF:], rs[:, :HALF] + rc[:, HALF:]], 1)
    col_re = jnp.concatenate([xc[:, :HALF] + xs[:, HALF:], xc[:, :HALF] - xs[:, HALF:]], 1)
    col_im = jnp.concatenate([xs[:, :HALF] - xc[:, HALF:], xs[:, :HALF] + xc[:, HALF:]], 1)
    top = lax.broadcasted_iota(jnp.int32, (16, 256), 0) == 0
    first_lane = lax.broadcasted_iota(jnp.int32, (HALF, HALF), 1) == 0
    for at, row, col in ((0, row_re, col_re), (256, row_im, col_im)):
        low = slice(at + HALF, at + HALF + 16)
        spec[low] = jnp.where(top, row, spec[low].astype(F32)).astype(BF16)
        for i in range(2):
            rows = slice(at + i * HALF, at + (i + 1) * HALF)
            stood = jnp.broadcast_to(col[:, i * HALF:(i + 1) * HALF], (HALF, HALF)).T
            spec[rows, HALF:] = jnp.where(first_lane, stood, spec[rows, HALF:].astype(F32)).astype(BF16)

    g_low = lax.broadcasted_iota(jnp.int32, (1, HALF), 1)
    g_all = jnp.concatenate([g_low, jnp.where(g_low == 0, -HALF, -g_low)], 1).astype(F32)
    infos = [c[HALF:SENT].astype(F32) for c in (c0, c1, c2, c3)]
    ends = [jnp.zeros((1, 1), F32)]

    def weight(s):
        i = s % 4
        return infos[s // 4][6 + i // 2:7 + i // 2, (i % 2) * HALF:(i % 2 + 1) * HALF]

    def propagate(s):
        passed = jnp.concatenate([spec[:256] * pupil[s], spec[256:] * pupil[s]], 0)
        k = jnp.dot(left[...], passed, preferred_element_type=F32)
        fields[s * HALF:(s + 1) * HALF, :256] = k[:HALF].astype(BF16)
        fields[s * HALF:(s + 1) * HALF, 256:] = k[HALF:].astype(BF16)
        b = infos[s // 4][2 + s % 4:3 + s % 4, HALF:]
        at = g_all + jnp.concatenate([b, b], 1)
        r, m = k[0:1], k[HALF:HALF + 1]
        pick = lambda x, v: jnp.sum(jnp.where(at == v, x, 0.0), axis=1, keepdims=True)
        z = pick(m, 64.0) * pick(r, -64.0) - pick(r, 64.0) * pick(m, -64.0)
        ends[0] = ends[0] + weight(s)[:, :1] * z

    def power(group):
        k = fields[group * 512:(group + 1) * 512, :]
        e_re = jnp.dot(k, right[0], preferred_element_type=F32)
        e_im = jnp.dot(k, right[1], preferred_element_type=F32)
        p = e_re * e_re + e_im * e_im
        parts = []
        for i in range(4):
            w = weight(group * 4 + i)
            parts.append(p[i * HALF:(i + 1) * HALF] * jnp.concatenate([w, w], 1))
        return (parts[0] + parts[1]) + (parts[2] + parts[3])

    summed = None
    for group in range(4):
        for s in range(4):
            propagate(group * 4 + s)
        if group:
            p = power(group - 1)
            summed = p if summed is None else summed + p
    summed = summed + power(3)
    high = summed.astype(BF16)
    low = (summed - high.astype(F32)).astype(BF16)
    tail = ends[0] * sine[0:1]
    copies = []
    for i in range(4):
        span = slice(i * 256, (i + 1) * 256)
        image[i] = (
            jnp.dot(high, spread[0, :, span], preferred_element_type=F32)
            + jnp.dot(low, spread[0, :, span], preferred_element_type=F32)
            + jnp.dot(high, spread[1, :, span], preferred_element_type=F32)
            + tail[:, span]
        )
        copies.append(pltpu.make_async_copy(image.at[i], out.at[:, span], sem.at[i]))
        copies[i].start()
    for copy in copies:
        copy.wait()


def inverse(*args):
    return pl.pallas_call(
        inverse_kernel,
        in_specs=[VMEM] * len(args),
        out_specs=pl.BlockSpec(memory_space=pltpu.HBM),
        out_shape=jax.ShapeDtypeStruct((HALF, NI), F32),
        scratch_shapes=[
            pltpu.VMEM((512, 256), BF16),
            pltpu.VMEM((8, 256), F32),
            pltpu.VMEM((2048, 512), BF16),
            pltpu.VMEM((4, HALF, 256), F32),
            pltpu.SemaphoreType.DMA((4,)),
        ],
        compiler_params=pltpu.CompilerParams(vmem_limit_bytes=24 * 1024 * 1024),
        cost_estimate=pl.CostEstimate(flops=2_500_000_000, bytes_accessed=3_000_000, transcendentals=0),
        name="inverse",
    )(*args)


def place_rows(left, place):
    freq = jnp.arange(256, dtype=jnp.int32)
    freq = jnp.where(freq < HALF, freq, jnp.where(freq == HALF, -HALF, HALF - freq))
    eighths = freq * place
    cos_q, sin_q = (x.astype(BF16) for x in quarter(jnp.right_shift(eighths, 1)))
    base = jnp.where(jnp.bitwise_and(eighths, 1) == 1, left[1], left[0])
    c, s = base[0] * cos_q - base[1] * sin_q, base[1] * cos_q + base[0] * sin_q
    return jnp.concatenate([jnp.concatenate([c, -s], 1), jnp.concatenate([s, c], 1)], 0)


def ring(x, k):
    return lax.ppermute(x, "src", [(i, (i + k) % 4) for i in range(4)])


def body(mask_clip, source_shifts, source_weights):
    table = forward_tables()
    left, right, spread, sine = inverse_tables()
    place = lax.axis_index("row") * 4 + lax.axis_index("src")
    left_mine = place_rows(jnp.asarray(left, BF16), place)
    far, after, before, keep = forward(mask_clip, source_shifts.T, source_weights, jnp.asarray(table, BF16))
    parts = [keep, ring(far, 2), ring(after, 1), ring(before, 3)]
    summed = small(add_kernel, "add", *parts)
    mine = small(finish_kernel, "finish", summed, lax.ppermute(summed, "row", [(0, 1), (1, 0)]))
    other = lax.ppermute(mine, "src", [(0, 1), (1, 0), (2, 3), (3, 2)])
    pupil, right, spread = pupils(parts, jnp.asarray(right, BF16), jnp.asarray(spread, BF16))
    return inverse(mine, other, *parts, pupil, left_mine, right, spread, jnp.asarray(sine, F32))


def solution(mesh):
    placed = (P(("clip", "row"), "src"), P("src", None), P("src"))
    return jax.shard_map(
        body, mesh=mesh, in_specs=placed, out_specs=P(("clip", "row", "src"), None), check_vma=False
    )
```

```python
import jax
import jax.numpy as jnp
import numpy as np
from jax import lax
from jax.experimental import pallas as pl
from jax.experimental.pallas import tpu as pltpu
from jax.sharding import PartitionSpec as P

NM = 4096
NI = 1024
TILE = NM // 4
HALF = 128
CHUNK = 512
QUARTER = 64
SENT = 136
COARSE = 256
NT = (((1,), (1,)), ((), ()))
F32 = jnp.float32
BF16 = jnp.bfloat16
VMEM = pl.BlockSpec(memory_space=pltpu.VMEM)


def forward_tables():
    freq = np.arange(HALF)
    pos = np.arange(TILE)
    angle = 2.0 * np.pi * ((freq[:, None] * pos[None, :]) % NM) / NM
    edge = 2.0 * np.pi * ((HALF * pos) % NM) / NM
    table = np.zeros((272, TILE), np.float64)
    table[:HALF] = np.cos(angle)
    table[HALF:256] = np.sin(angle)
    table[256] = np.cos(edge)
    table[257] = np.sin(edge)
    table[266, :HALF] = np.cos(edge[:HALF])
    table[267, :HALF] = np.sin(edge[:HALF])
    return (table / 64).astype(np.float32)


def inverse_tables():
    freq = np.concatenate([np.arange(HALF), -np.arange(HALF)])
    freq[HALF] = -HALF
    rows = np.arange(NI)
    angle = 2.0 * np.pi * ((rows[:, None] * freq[None, :]) % NI) / NI
    left = [np.stack([np.cos(angle[:HALF] + t), np.sin(angle[:HALF] + t)]) / 16 for t in (0.0, np.pi / 4)]
    left = np.stack(left)
    cos_y, sin_y = np.cos(angle[::4]).T / 64, np.sin(angle[::4]).T / 64
    right = np.stack([np.concatenate([cos_y, -sin_y], 0), np.concatenate([sin_y, cos_y], 0)])
    j = np.arange(COARSE)
    harmonic = np.arange(1, HALF)
    columns = np.arange(NI)
    distance = (columns[None, :] - 4 * j[:, None]) % NI
    lags = 2.0 * np.pi * ((np.arange(NI)[:, None] * harmonic[None, :]) % NI) / NI
    wave = (1.0 + 2.0 * np.cos(lags).sum(1) + np.cos(2.0 * np.pi * (np.arange(NI) * HALF % NI) / NI)) / COARSE
    spread = wave[distance]
    high = np.asarray(spread.astype(np.float32).astype(BF16), np.float64)
    spread = np.stack([high, spread - high])
    sine = np.zeros((8, NI), np.float64)
    sine[0] = -2.0 * np.sin(np.pi * (columns % 8) / 4) / 4096
    return tuple(x.astype(np.float32) for x in (left, right, spread, sine))


def quarter(turns):
    q = jnp.bitwise_and(turns, 3)
    cos_q = jnp.where(q == 0, 1.0, jnp.where(q == 2, -1.0, 0.0)).astype(F32)
    sin_q = jnp.where(q == 1, 1.0, jnp.where(q == 3, -1.0, 0.0)).astype(F32)
    return cos_q, sin_q


def forward_kernel(shifts_in, weights_in, mask, upright_in, table_in, far, after, before, keep,
                   shifts, weights, block, upright, table, half_way, folded, whole, sem):
    upright_copy = pltpu.make_async_copy(upright_in, upright, sem.at[0])
    late_copies = [
        pltpu.make_async_copy(table_in, table, sem.at[1]),
        pltpu.make_async_copy(shifts_in, shifts, sem.at[2]),
        pltpu.make_async_copy(weights_in, weights, sem.at[7]),
    ]
    copies = [
        pltpu.make_async_copy(
            mask.at[i * CHUNK:(i + 1) * CHUNK], block.at[i * CHUNK:(i + 1) * CHUNK], sem.at[3 + i]
        )
        for i in range(4)
    ]
    for copy in (upright_copy, *copies, *late_copies):
        copy.start()
    row_id = lax.axis_index("row")
    src_id = lax.axis_index("src")
    f_col = lax.broadcasted_iota(jnp.int32, (HALF, 256), 0)
    cos_f, sin_f = quarter(f_col)
    sign, _ = quarter(f_col * 2 * row_id)
    cos_g, sin_g = quarter(lax.broadcasted_iota(jnp.int32, (HALF, HALF), 1) * src_id)

    def join_rows(a, b):
        top = (a[:HALF] + cos_f * b[:HALF] - sin_f * b[HALF:256]) * sign
        low = (a[HALF:256] + cos_f * b[HALF:256] + sin_f * b[:HALF]) * sign
        return top, low

    def turn_columns(x):
        c, s = cos_g[:x.shape[0]], sin_g[:x.shape[0]]
        return c * x[:, :HALF] - s * x[:, HALF:], c * x[:, HALF:] + s * x[:, :HALF]

    upright_copy.wait()

    @pl.loop(0, 4)
    def _(i):
        rows = pl.ds(pl.multiple_of(i * CHUNK, CHUNK), CHUNK)
        pltpu.make_async_copy(mask.at[rows], block.at[rows], sem.at[3 + i]).wait()
        half_way[rows] = jnp.dot(
            block[rows], upright[...], preferred_element_type=F32
        ).astype(BF16)
        lanes = pl.ds(pl.multiple_of((i // 2) * HALF, HALF), HALF)
        for low in range(0, CHUNK, 64):
            strip = pl.ds(pl.multiple_of(i * CHUNK + low, 64), 64)
            tiles = [block[strip, tile * HALF:(tile + 1) * HALF] for tile in range(8)]
            while len(tiles) > 1:
                tiles = [tiles[t] + tiles[t + 1] for t in range(0, len(tiles), 2)]
            folded[pl.ds(pl.multiple_of(lax.rem(i, 2) * CHUNK + low, 64), 64), lanes] = tiles[0]

    for copy in late_copies:
        copy.wait()
    sums = [
        jnp.dot(table[:264], half_way[h * TILE:(h + 1) * TILE], preferred_element_type=F32)
        for h in range(2)
    ]
    sides = jnp.dot(table[:256, :], folded[...], preferred_element_type=F32)
    a, b = sums
    for start, x in zip((0, HALF), join_rows(a, b)):
        x_cos, x_sin = turn_columns(x)
        whole[start:start + HALF, :HALF] = x_cos
        whole[start:start + HALF, HALF:] = x_sin
    e_cos, e_sin = turn_columns(a[256:] + b[256:])
    s_a, s_b = sides[:, :HALF], sides[:, HALF:]
    c, s, g = cos_f[:, :HALF], sin_f[:, :HALF], sign[:, :HALF]
    edges = jnp.concatenate(
        [
            (s_a[:HALF] + c * s_b[:HALF] - s * s_b[HALF:]) * g,
            (s_a[HALF:] + c * s_b[HALF:] + s * s_b[:HALF]) * g,
        ],
        0,
    ).astype(BF16)
    crossed = lax.dot_general(table[264:272, :HALF], edges, NT, preferred_element_type=F32)
    edges = jnp.concatenate([e_cos + crossed[:, :HALF], e_sin + crossed[:, HALF:]], 1)
    row = lax.broadcasted_iota(jnp.int32, (8, HALF), 0)
    first = jnp.zeros((8, HALF), F32)
    second = jnp.zeros((8, HALF), F32)
    for i in range(4):
        first = jnp.where(row == 2 + i, shifts[0, i].astype(F32), first)
        second = jnp.where(row == 2 + i, shifts[1, i].astype(F32), second)
        w = weights[i].astype(F32)
        if i % 2 == 0:
            first = jnp.where(row == 6 + i // 2, w, first)
        else:
            second = jnp.where(row == 6 + i // 2, w, second)
    sources = jnp.concatenate([first, second], 1)
    row = lax.broadcasted_iota(jnp.int32, (8, 256), 0)
    for outs, odd in (((far, keep), lax.rem(src_id, 2)), ((after, before), lax.rem(src_id + 1, 2))):
        at = pl.multiple_of(odd * QUARTER, QUARTER)
        lines = [jnp.where(odd == 1, edges[2 + i:3 + i], edges[i:i + 1]) for i in range(2)]
        rows = jnp.where(row == 0, lines[0], jnp.where(row == 1, lines[1], sources)).astype(BF16)
        cos_rows = whole[pl.ds(at, QUARTER)].astype(BF16)
        sin_rows = whole[pl.ds(HALF + at, QUARTER)].astype(BF16)
        for out in outs:
            out[:QUARTER] = cos_rows
            out[QUARTER:HALF] = sin_rows
            out[HALF:SENT] = rows


def forward(mask_clip, shifts, weights, upright, table):
    hbm = pl.BlockSpec(memory_space=pltpu.HBM)
    return pl.pallas_call(
        forward_kernel,
        in_specs=[hbm] * 5,
        out_specs=[VMEM] * 4,
        out_shape=[jax.ShapeDtypeStruct((SENT, 256), BF16)] * 4,
        scratch_shapes=[
            pltpu.SMEM((2, 4), jnp.int32),
            pltpu.SMEM((4,), jnp.int32),
            pltpu.VMEM((2 * TILE, TILE), BF16),
            pltpu.VMEM((TILE, 256), BF16),
            pltpu.VMEM((272, TILE), BF16),
            pltpu.VMEM((2 * TILE, 256), BF16),
            pltpu.VMEM((TILE, 256), BF16),
            pltpu.VMEM((256, 256), F32),
            pltpu.SemaphoreType.DMA((8,)),
        ],
        compiler_params=pltpu.CompilerParams(vmem_limit_bytes=16 * 1024 * 1024),
        cost_estimate=pl.CostEstimate(flops=1_700_000_000, bytes_accessed=5_000_000, transcendentals=0),
        name="forward",
    )(*[pltpu.with_memory_space_constraint(x, pltpu.HBM) for x in (shifts, weights, mask_clip, upright, table)])


def add_kernel(own, one, two, three, out):
    out[...] = (
        own[...].astype(F32) + one[...].astype(F32) + two[...].astype(F32) + three[...].astype(F32)
    ).astype(BF16)


def finish_kernel(mine, other, out):
    total = mine[...].astype(F32) + other[...].astype(F32)
    cc, cs = total[:QUARTER, :HALF], total[:QUARTER, HALF:]
    sc, ss = total[QUARTER:HALF, :HALF], total[QUARTER:HALF, HALF:]
    out[:QUARTER, :HALF] = (cc - ss).astype(BF16)
    out[:QUARTER, HALF:] = (cc + ss).astype(BF16)
    out[QUARTER:HALF, :HALF] = (-(sc + cs)).astype(BF16)
    out[QUARTER:HALF, HALF:] = (cs - sc).astype(BF16)
    out[HALF:] = total[HALF:].astype(BF16)


def small(kernel, name, *args):
    return pl.pallas_call(
        kernel,
        in_specs=[VMEM] * len(args),
        out_specs=VMEM,
        out_shape=jax.ShapeDtypeStruct((SENT, 256), BF16),
        compiler_params=pltpu.CompilerParams(vmem_limit_bytes=4 * 1024 * 1024),
        name=name,
    )(*args)


def pupil_kernel(c0, c1, c2, c3, right_in, spread_in, out, right, spread, sem):
    copies = [
        pltpu.make_async_copy(right_in, right, sem.at[0]),
        pltpu.make_async_copy(spread_in, spread, sem.at[1]),
    ]
    for copy in copies:
        copy.start()
    f_low = lax.broadcasted_iota(jnp.int32, (HALF, HALF), 0)
    g_low = lax.broadcasted_iota(jnp.int32, (1, HALF), 1)
    f_halves = (f_low.astype(F32), jnp.where(f_low == 0, -HALF, -f_low).astype(F32))
    g_halves = (g_low.astype(F32), jnp.where(g_low == 0, -HALF, -g_low).astype(F32))
    for s in range(16):
        info = (c0, c1, c2, c3)[s // 4][HALF:SENT].astype(F32)
        i = 2 + s % 4
        a, b = info[i:i + 1, :HALF], info[i:i + 1, HALF:]
        for i, f in enumerate(f_halves):
            room = 4096.0 - (f + a) * (f + a)
            for j, g in enumerate(g_halves):
                reach = (g + b) * (g + b)
                out[s, i * HALF:(i + 1) * HALF, j * HALF:(j + 1) * HALF] = jnp.where(
                    room >= reach, 1.0, 0.0
                ).astype(BF16)
    for copy in copies:
        copy.wait()


def pupils(parts, right, spread):
    tables = [pltpu.with_memory_space_constraint(x, pltpu.HBM) for x in (right, spread)]
    return pl.pallas_call(
        pupil_kernel,
        in_specs=[VMEM] * 4 + [pl.BlockSpec(memory_space=pltpu.HBM)] * 2,
        out_specs=[VMEM] * 3,
        out_shape=[
            jax.ShapeDtypeStruct((16, 256, 256), BF16),
            jax.ShapeDtypeStruct(right.shape, BF16),
            jax.ShapeDtypeStruct(spread.shape, BF16),
        ],
        scratch_shapes=[pltpu.SemaphoreType.DMA((2,))],
        compiler_params=pltpu.CompilerParams(vmem_limit_bytes=8 * 1024 * 1024),
        cost_estimate=pl.CostEstimate(flops=10_000_000, bytes_accessed=4_000_000, transcendentals=0),
        name="pupils",
    )(*parts, *tables)


def inverse_kernel(mine, other, c0, c1, c2, c3, pupil, left, right, spread, sine, out,
                   spec, edge, fields, image, sem):
    src_id = lax.axis_index("src")
    for chunk, odd in ((mine, lax.rem(src_id, 2)), (other, lax.rem(src_id + 1, 2))):
        at = pl.multiple_of(odd * QUARTER, QUARTER)
        re, im = chunk[:QUARTER], chunk[QUARTER:HALF]
        spec[pl.ds(at, QUARTER)] = re
        spec[pl.ds(256 + at, QUARTER)] = im
        spec[pl.ds(HALF + at, QUARTER), :HALF] = re[:, HALF:]
        spec[pl.ds(HALF + at, QUARTER), HALF:] = re[:, :HALF]
        spec[pl.ds(384 + at, QUARTER), :HALF] = -im[:, HALF:]
        spec[pl.ds(384 + at, QUARTER), HALF:] = -im[:, :HALF]
        lines = chunk[HALF:SENT].astype(F32)
        edge[pl.ds(odd * 2, 1)] = lines[0:1]
        edge[pl.ds(odd * 2 + 1, 1)] = lines[1:2]
    rc, rs, xc, xs = (edge[i:i + 1] for i in range(4))
    row_re = jnp.concatenate([rc[:, :HALF] + rs[:, HALF:], rc[:, :HALF] - rs[:, HALF:]], 1)
    row_im = jnp.concatenate([rs[:, :HALF] - rc[:, HALF:], rs[:, :HALF] + rc[:, HALF:]], 1)
    col_re = jnp.concatenate([xc[:, :HALF] + xs[:, HALF:], xc[:, :HALF] - xs[:, HALF:]], 1)
    col_im = jnp.concatenate([xs[:, :HALF] - xc[:, HALF:], xs[:, :HALF] + xc[:, HALF:]], 1)
    top = lax.broadcasted_iota(jnp.int32, (16, 256), 0) == 0
    first_lane = lax.broadcasted_iota(jnp.int32, (HALF, HALF), 1) == 0
    for at, row, col in ((0, row_re, col_re), (256, row_im, col_im)):
        low = slice(at + HALF, at + HALF + 16)
        spec[low] = jnp.where(top, row, spec[low].astype(F32)).astype(BF16)
        for i in range(2):
            rows = slice(at + i * HALF, at + (i + 1) * HALF)
            stood = jnp.broadcast_to(col[:, i * HALF:(i + 1) * HALF], (HALF, HALF)).T
            spec[rows, HALF:] = jnp.where(first_lane, stood, spec[rows, HALF:].astype(F32)).astype(BF16)

    g_low = lax.broadcasted_iota(jnp.int32, (1, HALF), 1)
    g_all = jnp.concatenate([g_low, jnp.where(g_low == 0, -HALF, -g_low)], 1).astype(F32)
    infos = [c[HALF:SENT].astype(F32) for c in (c0, c1, c2, c3)]
    ends = [jnp.zeros((1, 1), F32)]

    def weight(s):
        i = s % 4
        return infos[s // 4][6 + i // 2:7 + i // 2, (i % 2) * HALF:(i % 2 + 1) * HALF]

    def propagate(s):
        passed = jnp.concatenate([spec[:256] * pupil[s], spec[256:] * pupil[s]], 0)
        k = jnp.dot(left[...], passed, preferred_element_type=F32)
        fields[s * HALF:(s + 1) * HALF, :256] = k[:HALF].astype(BF16)
        fields[s * HALF:(s + 1) * HALF, 256:] = k[HALF:].astype(BF16)
        b = infos[s // 4][2 + s % 4:3 + s % 4, HALF:]
        at = g_all + jnp.concatenate([b, b], 1)
        r, m = k[0:1], k[HALF:HALF + 1]
        pick = lambda x, v: jnp.sum(jnp.where(at == v, x, 0.0), axis=1, keepdims=True)
        z = pick(m, 64.0) * pick(r, -64.0) - pick(r, 64.0) * pick(m, -64.0)
        ends[0] = ends[0] + weight(s)[:, :1] * z

    def power(group):
        k = fields[group * 512:(group + 1) * 512, :]
        e_re = jnp.dot(k, right[0], preferred_element_type=F32)
        e_im = jnp.dot(k, right[1], preferred_element_type=F32)
        p = e_re * e_re + e_im * e_im
        parts = []
        for i in range(4):
            w = weight(group * 4 + i)
            parts.append(p[i * HALF:(i + 1) * HALF] * jnp.concatenate([w, w], 1))
        return (parts[0] + parts[1]) + (parts[2] + parts[3])

    summed = None
    for group in range(4):
        for s in range(4):
            propagate(group * 4 + s)
        if group:
            p = power(group - 1)
            summed = p if summed is None else summed + p
    summed = summed + power(3)
    high = summed.astype(BF16)
    low = (summed - high.astype(F32)).astype(BF16)
    tail = ends[0] * sine[0:1]
    copies = []
    for i in range(4):
        span = slice(i * 256, (i + 1) * 256)
        image[i] = (
            jnp.dot(high, spread[0, :, span], preferred_element_type=F32)
            + jnp.dot(low, spread[0, :, span], preferred_element_type=F32)
            + jnp.dot(high, spread[1, :, span], preferred_element_type=F32)
            + tail[:, span]
        )
        copies.append(pltpu.make_async_copy(image.at[i], out.at[:, span], sem.at[i]))
        copies[i].start()
    for copy in copies:
        copy.wait()


def inverse(*args):
    return pl.pallas_call(
        inverse_kernel,
        in_specs=[VMEM] * len(args),
        out_specs=pl.BlockSpec(memory_space=pltpu.HBM),
        out_shape=jax.ShapeDtypeStruct((HALF, NI), F32),
        scratch_shapes=[
            pltpu.VMEM((512, 256), BF16),
            pltpu.VMEM((8, 256), F32),
            pltpu.VMEM((2048, 512), BF16),
            pltpu.VMEM((4, HALF, 256), F32),
            pltpu.SemaphoreType.DMA((4,)),
        ],
        compiler_params=pltpu.CompilerParams(vmem_limit_bytes=24 * 1024 * 1024),
        cost_estimate=pl.CostEstimate(flops=2_500_000_000, bytes_accessed=3_000_000, transcendentals=0),
        name="inverse",
    )(*args)


def place_rows(left, place):
    freq = jnp.arange(256, dtype=jnp.int32)
    freq = jnp.where(freq < HALF, freq, jnp.where(freq == HALF, -HALF, HALF - freq))
    eighths = freq * place
    cos_q, sin_q = (x.astype(BF16) for x in quarter(jnp.right_shift(eighths, 1)))
    base = jnp.where(jnp.bitwise_and(eighths, 1) == 1, left[1], left[0])
    c, s = base[0] * cos_q - base[1] * sin_q, base[1] * cos_q + base[0] * sin_q
    return jnp.concatenate([jnp.concatenate([c, -s], 1), jnp.concatenate([s, c], 1)], 0)


def ring(x, k):
    return lax.ppermute(x, "src", [(i, (i + k) % 4) for i in range(4)])


def body(mask_clip, source_shifts, source_weights):
    table = forward_tables()
    left, right, spread, sine = inverse_tables()
    place = lax.axis_index("row") * 4 + lax.axis_index("src")
    left_mine = place_rows(jnp.asarray(left, BF16), place)
    far, after, before, keep = forward(
        mask_clip,
        source_shifts.T,
        source_weights,
        jnp.asarray(table[:256].T, BF16),
        jnp.asarray(table, BF16),
    )
    parts = [keep, ring(far, 2), ring(after, 1), ring(before, 3)]
    summed = small(add_kernel, "add", *parts)
    mine = small(finish_kernel, "finish", summed, lax.ppermute(summed, "row", [(0, 1), (1, 0)]))
    other = lax.ppermute(mine, "src", [(0, 1), (1, 0), (2, 3), (3, 2)])
    pupil, right, spread = pupils(parts, jnp.asarray(right, BF16), jnp.asarray(spread, BF16))
    return inverse(mine, other, *parts, pupil, left_mine, right, spread, jnp.asarray(sine, F32))


def solution(mesh):
    placed = (P(("clip", "row"), "src"), P("src", None), P("src"))
    return jax.shard_map(
        body, mesh=mesh, in_specs=placed, out_specs=P(("clip", "row", "src"), None), check_vma=False
    )
```

```python
import jax
import jax.numpy as jnp
import numpy as np
from jax import lax
from jax.experimental import pallas as pl
from jax.experimental.pallas import tpu as pltpu
from jax.sharding import PartitionSpec as P

NM = 4096
NI = 1024
TILE = NM // 4
HALF = 128
CHUNK = 512
QUARTER = 64
SENT = 136
COARSE = 256
NT = (((1,), (1,)), ((), ()))
F32 = jnp.float32
BF16 = jnp.bfloat16
VMEM = pl.BlockSpec(memory_space=pltpu.VMEM)


def forward_tables():
    freq = np.arange(HALF)
    pos = np.arange(TILE)
    angle = 2.0 * np.pi * ((freq[:, None] * pos[None, :]) % NM) / NM
    edge = 2.0 * np.pi * ((HALF * pos) % NM) / NM
    table = np.zeros((272, TILE), np.float64)
    table[:HALF] = np.cos(angle)
    table[HALF:256] = np.sin(angle)
    table[256] = np.cos(edge)
    table[257] = np.sin(edge)
    table[266, :HALF] = np.cos(edge[:HALF])
    table[267, :HALF] = np.sin(edge[:HALF])
    return (table / 64).astype(np.float32)


def inverse_tables():
    freq = np.concatenate([np.arange(HALF), -np.arange(HALF)])
    freq[HALF] = -HALF
    rows = np.arange(NI)
    angle = 2.0 * np.pi * ((rows[:, None] * freq[None, :]) % NI) / NI
    left = [np.stack([np.cos(angle[:HALF] + t), np.sin(angle[:HALF] + t)]) / 16 for t in (0.0, np.pi / 4)]
    left = np.stack(left)
    cos_y, sin_y = np.cos(angle[::4]).T / 64, np.sin(angle[::4]).T / 64
    right = np.stack([np.concatenate([cos_y, -sin_y], 0), np.concatenate([sin_y, cos_y], 0)])
    j = np.arange(COARSE)
    harmonic = np.arange(1, HALF)
    columns = np.arange(NI)
    distance = (columns[None, :] - 4 * j[:, None]) % NI
    lags = 2.0 * np.pi * ((np.arange(NI)[:, None] * harmonic[None, :]) % NI) / NI
    wave = (1.0 + 2.0 * np.cos(lags).sum(1) + np.cos(2.0 * np.pi * (np.arange(NI) * HALF % NI) / NI)) / COARSE
    spread = wave[distance]
    high = np.asarray(spread.astype(np.float32).astype(BF16), np.float64)
    spread = np.stack([high, spread - high])
    sine = np.zeros((8, NI), np.float64)
    sine[0] = -2.0 * np.sin(np.pi * (columns % 8) / 4) / 4096
    return tuple(x.astype(np.float32) for x in (left, right, spread, sine))


def quarter(turns):
    q = jnp.bitwise_and(turns, 3)
    cos_q = jnp.where(q == 0, 1.0, jnp.where(q == 2, -1.0, 0.0)).astype(F32)
    sin_q = jnp.where(q == 1, 1.0, jnp.where(q == 3, -1.0, 0.0)).astype(F32)
    return cos_q, sin_q


def forward_kernel(shifts_in, weights_in, mask, upright_in, table_in, far, after, before, keep,
                   shifts, weights, block, upright, table, half_way, folded, whole, sem):
    upright_copy = pltpu.make_async_copy(upright_in, upright, sem.at[0])
    late_copies = [
        pltpu.make_async_copy(table_in, table, sem.at[1]),
        pltpu.make_async_copy(shifts_in, shifts, sem.at[2]),
        pltpu.make_async_copy(weights_in, weights, sem.at[7]),
    ]
    copies = [
        pltpu.make_async_copy(
            mask.at[i * CHUNK:(i + 1) * CHUNK], block.at[i * CHUNK:(i + 1) * CHUNK], sem.at[3 + i]
        )
        for i in range(4)
    ]
    for copy in (upright_copy, *copies, *late_copies):
        copy.start()
    row_id = lax.axis_index("row")
    src_id = lax.axis_index("src")
    f_col = lax.broadcasted_iota(jnp.int32, (HALF, 256), 0)
    cos_f, sin_f = quarter(f_col)
    sign, _ = quarter(f_col * 2 * row_id)
    cos_g, sin_g = quarter(lax.broadcasted_iota(jnp.int32, (HALF, HALF), 1) * src_id)

    def join_rows(a, b):
        top = (a[:HALF] + cos_f * b[:HALF] - sin_f * b[HALF:256]) * sign
        low = (a[HALF:256] + cos_f * b[HALF:256] + sin_f * b[:HALF]) * sign
        return top, low

    def turn_columns(x):
        c, s = cos_g[:x.shape[0]], sin_g[:x.shape[0]]
        return c * x[:, :HALF] - s * x[:, HALF:], c * x[:, HALF:] + s * x[:, :HALF]

    upright_copy.wait()

    @pl.loop(0, 4)
    def _(i):
        rows = pl.ds(pl.multiple_of(i * CHUNK, CHUNK), CHUNK)
        pltpu.make_async_copy(mask.at[rows], block.at[rows], sem.at[3 + i]).wait()
        half_way[rows] = jnp.dot(
            block[rows], upright[...], preferred_element_type=F32
        ).astype(BF16)
        lanes = pl.ds(pl.multiple_of((i // 2) * HALF, HALF), HALF)
        for low in range(0, CHUNK, 64):
            strip = pl.ds(pl.multiple_of(i * CHUNK + low, 64), 64)
            tiles = [block[strip, tile * HALF:(tile + 1) * HALF] for tile in range(8)]
            while len(tiles) > 1:
                tiles = [tiles[t] + tiles[t + 1] for t in range(0, len(tiles), 2)]
            folded[pl.ds(pl.multiple_of(lax.rem(i, 2) * CHUNK + low, 64), 64), lanes] = tiles[0]

    for copy in late_copies:
        copy.wait()
    sums = [
        jnp.dot(table[:264], half_way[h * TILE:(h + 1) * TILE], preferred_element_type=F32)
        for h in range(2)
    ]
    sides = jnp.dot(table[:256, :], folded[...], preferred_element_type=F32)
    a, b = sums
    for start, x in zip((0, HALF), join_rows(a, b)):
        x_cos, x_sin = turn_columns(x)
        whole[start:start + HALF, :HALF] = x_cos
        whole[start:start + HALF, HALF:] = x_sin
    e_cos, e_sin = turn_columns(a[256:] + b[256:])
    s_a, s_b = sides[:, :HALF], sides[:, HALF:]
    c, s, g = cos_f[:, :HALF], sin_f[:, :HALF], sign[:, :HALF]
    edges = jnp.concatenate(
        [
            (s_a[:HALF] + c * s_b[:HALF] - s * s_b[HALF:]) * g,
            (s_a[HALF:] + c * s_b[HALF:] + s * s_b[:HALF]) * g,
        ],
        0,
    ).astype(BF16)
    crossed = lax.dot_general(table[264:272, :HALF], edges, NT, preferred_element_type=F32)
    edges = jnp.concatenate([e_cos + crossed[:, :HALF], e_sin + crossed[:, HALF:]], 1)
    row = lax.broadcasted_iota(jnp.int32, (8, HALF), 0)
    first = jnp.zeros((8, HALF), F32)
    second = jnp.zeros((8, HALF), F32)
    for i in range(4):
        first = jnp.where(row == 2 + i, shifts[0, i].astype(F32), first)
        second = jnp.where(row == 2 + i, shifts[1, i].astype(F32), second)
        w = weights[i].astype(F32)
        if i % 2 == 0:
            first = jnp.where(row == 6 + i // 2, w, first)
        else:
            second = jnp.where(row == 6 + i // 2, w, second)
    sources = jnp.concatenate([first, second], 1)
    row = lax.broadcasted_iota(jnp.int32, (8, 256), 0)
    for outs, odd in (((far, keep), lax.rem(src_id, 2)), ((after, before), lax.rem(src_id + 1, 2))):
        at = pl.multiple_of(odd * QUARTER, QUARTER)
        lines = [jnp.where(odd == 1, edges[2 + i:3 + i], edges[i:i + 1]) for i in range(2)]
        rows = jnp.where(row == 0, lines[0], jnp.where(row == 1, lines[1], sources)).astype(BF16)
        cos_rows = whole[pl.ds(at, QUARTER)].astype(BF16)
        sin_rows = whole[pl.ds(HALF + at, QUARTER)].astype(BF16)
        for out in outs:
            out[:QUARTER] = cos_rows
            out[QUARTER:HALF] = sin_rows
            out[HALF:SENT] = rows


def forward(mask_clip, shifts, weights, upright, table):
    hbm = pl.BlockSpec(memory_space=pltpu.HBM)
    return pl.pallas_call(
        forward_kernel,
        in_specs=[hbm] * 5,
        out_specs=[VMEM] * 4,
        out_shape=[jax.ShapeDtypeStruct((SENT, 256), BF16)] * 4,
        scratch_shapes=[
            pltpu.SMEM((2, 4), jnp.int32),
            pltpu.SMEM((4,), jnp.int32),
            pltpu.VMEM((2 * TILE, TILE), BF16),
            pltpu.VMEM((TILE, 256), BF16),
            pltpu.VMEM((272, TILE), BF16),
            pltpu.VMEM((2 * TILE, 256), BF16),
            pltpu.VMEM((TILE, 256), BF16),
            pltpu.VMEM((256, 256), F32),
            pltpu.SemaphoreType.DMA((8,)),
        ],
        compiler_params=pltpu.CompilerParams(vmem_limit_bytes=16 * 1024 * 1024),
        cost_estimate=pl.CostEstimate(flops=1_700_000_000, bytes_accessed=5_000_000, transcendentals=0),
        name="forward",
    )(*[pltpu.with_memory_space_constraint(x, pltpu.HBM) for x in (shifts, weights, mask_clip, upright, table)])


def add_kernel(own, one, two, three, out):
    out[...] = (
        own[...].astype(F32) + one[...].astype(F32) + two[...].astype(F32) + three[...].astype(F32)
    ).astype(BF16)


def finish_kernel(mine, other, out):
    total = mine[...].astype(F32) + other[...].astype(F32)
    cc, cs = total[:QUARTER, :HALF], total[:QUARTER, HALF:]
    sc, ss = total[QUARTER:HALF, :HALF], total[QUARTER:HALF, HALF:]
    out[:QUARTER, :HALF] = (cc - ss).astype(BF16)
    out[:QUARTER, HALF:] = (cc + ss).astype(BF16)
    out[QUARTER:HALF, :HALF] = (-(sc + cs)).astype(BF16)
    out[QUARTER:HALF, HALF:] = (cs - sc).astype(BF16)
    out[HALF:] = total[HALF:].astype(BF16)


def small(kernel, name, *args):
    return pl.pallas_call(
        kernel,
        in_specs=[VMEM] * len(args),
        out_specs=VMEM,
        out_shape=jax.ShapeDtypeStruct((SENT, 256), BF16),
        compiler_params=pltpu.CompilerParams(vmem_limit_bytes=4 * 1024 * 1024),
        name=name,
    )(*args)


def pupil_kernel(c0, c1, c2, c3, right_in, spread_in, out, right, spread, sem):
    copies = [
        pltpu.make_async_copy(right_in, right, sem.at[0]),
        pltpu.make_async_copy(spread_in, spread, sem.at[1]),
    ]
    for copy in copies:
        copy.start()
    f_low = lax.broadcasted_iota(jnp.int32, (HALF, HALF), 0)
    g_low = lax.broadcasted_iota(jnp.int32, (1, HALF), 1)
    f_halves = (f_low.astype(F32), jnp.where(f_low == 0, -HALF, -f_low).astype(F32))
    g_halves = (g_low.astype(F32), jnp.where(g_low == 0, -HALF, -g_low).astype(F32))
    for s in range(16):
        info = (c0, c1, c2, c3)[s // 4][HALF:SENT].astype(F32)
        i = 2 + s % 4
        a, b = info[i:i + 1, :HALF], info[i:i + 1, HALF:]
        for i, f in enumerate(f_halves):
            room = 4096.0 - (f + a) * (f + a)
            for j, g in enumerate(g_halves):
                reach = (g + b) * (g + b)
                out[s, i * HALF:(i + 1) * HALF, j * HALF:(j + 1) * HALF] = jnp.where(
                    room >= reach, 1.0, 0.0
                ).astype(BF16)
    for copy in copies:
        copy.wait()


def pupils(parts, right, spread):
    tables = [pltpu.with_memory_space_constraint(x, pltpu.HBM) for x in (right, spread)]
    return pl.pallas_call(
        pupil_kernel,
        in_specs=[VMEM] * 4 + [pl.BlockSpec(memory_space=pltpu.HBM)] * 2,
        out_specs=[VMEM] * 3,
        out_shape=[
            jax.ShapeDtypeStruct((16, 256, 256), BF16),
            jax.ShapeDtypeStruct(right.shape, BF16),
            jax.ShapeDtypeStruct(spread.shape, BF16),
        ],
        scratch_shapes=[pltpu.SemaphoreType.DMA((2,))],
        compiler_params=pltpu.CompilerParams(vmem_limit_bytes=8 * 1024 * 1024),
        cost_estimate=pl.CostEstimate(flops=10_000_000, bytes_accessed=4_000_000, transcendentals=0),
        name="pupils",
    )(*parts, *tables)


def inverse_kernel(mine, other, c0, c1, c2, c3, pupil, left, right, spread, sine, out,
                   spec, edge, fields, image, sem):
    src_id = lax.axis_index("src")
    for chunk, odd in ((mine, lax.rem(src_id, 2)), (other, lax.rem(src_id + 1, 2))):
        at = pl.multiple_of(odd * QUARTER, QUARTER)
        re, im = chunk[:QUARTER], chunk[QUARTER:HALF]
        spec[pl.ds(at, QUARTER)] = re
        spec[pl.ds(256 + at, QUARTER)] = im
        spec[pl.ds(HALF + at, QUARTER), :HALF] = re[:, HALF:]
        spec[pl.ds(HALF + at, QUARTER), HALF:] = re[:, :HALF]
        spec[pl.ds(384 + at, QUARTER), :HALF] = -im[:, HALF:]
        spec[pl.ds(384 + at, QUARTER), HALF:] = -im[:, :HALF]
        lines = chunk[HALF:SENT].astype(F32)
        edge[pl.ds(odd * 2, 1)] = lines[0:1]
        edge[pl.ds(odd * 2 + 1, 1)] = lines[1:2]
    rc, rs, xc, xs = (edge[i:i + 1] for i in range(4))
    row_re = jnp.concatenate([rc[:, :HALF] + rs[:, HALF:], rc[:, :HALF] - rs[:, HALF:]], 1)
    row_im = jnp.concatenate([rs[:, :HALF] - rc[:, HALF:], rs[:, :HALF] + rc[:, HALF:]], 1)
    col_re = jnp.concatenate([xc[:, :HALF] + xs[:, HALF:], xc[:, :HALF] - xs[:, HALF:]], 1)
    col_im = jnp.concatenate([xs[:, :HALF] - xc[:, HALF:], xs[:, :HALF] + xc[:, HALF:]], 1)
    top = lax.broadcasted_iota(jnp.int32, (16, 256), 0) == 0
    first_lane = lax.broadcasted_iota(jnp.int32, (HALF, HALF), 1) == 0
    for at, row, col in ((0, row_re, col_re), (256, row_im, col_im)):
        low = slice(at + HALF, at + HALF + 16)
        spec[low] = jnp.where(top, row, spec[low].astype(F32)).astype(BF16)
        for i in range(2):
            rows = slice(at + i * HALF, at + (i + 1) * HALF)
            stood = jnp.broadcast_to(col[:, i * HALF:(i + 1) * HALF], (HALF, HALF)).T
            spec[rows, HALF:] = jnp.where(first_lane, stood, spec[rows, HALF:].astype(F32)).astype(BF16)

    g_low = lax.broadcasted_iota(jnp.int32, (1, HALF), 1)
    g_all = jnp.concatenate([g_low, jnp.where(g_low == 0, -HALF, -g_low)], 1).astype(F32)
    infos = [c[HALF:SENT].astype(F32) for c in (c0, c1, c2, c3)]
    ends = [jnp.zeros((1, 1), F32)]

    def weight(s):
        i = s % 4
        return infos[s // 4][6 + i // 2:7 + i // 2, (i % 2) * HALF:(i % 2 + 1) * HALF]

    def propagate(s):
        passed = jnp.concatenate([spec[:256] * pupil[s], spec[256:] * pupil[s]], 0)
        k = jnp.dot(left[...], passed, preferred_element_type=F32)
        fields[s * HALF:(s + 1) * HALF, :256] = k[:HALF].astype(BF16)
        fields[s * HALF:(s + 1) * HALF, 256:] = k[HALF:].astype(BF16)
        b = infos[s // 4][2 + s % 4:3 + s % 4, HALF:]
        at = g_all + jnp.concatenate([b, b], 1)
        r, m = k[0:1], k[HALF:HALF + 1]
        pick = lambda x, v: jnp.sum(jnp.where(at == v, x, 0.0), axis=1, keepdims=True)
        z = pick(m, 64.0) * pick(r, -64.0) - pick(r, 64.0) * pick(m, -64.0)
        ends[0] = ends[0] + weight(s)[:, :1] * z

    def power(group):
        k = fields[group * 512:(group + 1) * 512, :]
        e_re = jnp.dot(k, right[0], preferred_element_type=F32)
        e_im = jnp.dot(k, right[1], preferred_element_type=F32)
        p = e_re * e_re + e_im * e_im
        parts = []
        for i in range(4):
            w = weight(group * 4 + i)
            parts.append(p[i * HALF:(i + 1) * HALF] * jnp.concatenate([w, w], 1))
        return (parts[0] + parts[1]) + (parts[2] + parts[3])

    summed = None
    for group in range(4):
        for s in range(4):
            propagate(group * 4 + s)
        if group:
            p = power(group - 1)
            summed = p if summed is None else summed + p
    summed = summed + power(3)
    high = summed.astype(BF16)
    low = (summed - high.astype(F32)).astype(BF16)
    tail = ends[0] * sine[0:1]
    copies = []
    for i in range(4):
        span = slice(i * 256, (i + 1) * 256)
        image[i] = (
            jnp.dot(high, spread[0, :, span], preferred_element_type=F32)
            + jnp.dot(low, spread[0, :, span], preferred_element_type=F32)
            + jnp.dot(high, spread[1, :, span], preferred_element_type=F32)
            + tail[:, span]
        )
        copies.append(pltpu.make_async_copy(image.at[i], out.at[:, span], sem.at[i]))
        copies[i].start()
    for copy in copies:
        copy.wait()


def inverse(*args):
    return pl.pallas_call(
        inverse_kernel,
        in_specs=[VMEM] * len(args),
        out_specs=pl.BlockSpec(memory_space=pltpu.HBM),
        out_shape=jax.ShapeDtypeStruct((HALF, NI), F32),
        scratch_shapes=[
            pltpu.VMEM((512, 256), BF16),
            pltpu.VMEM((8, 256), F32),
            pltpu.VMEM((2048, 512), BF16),
            pltpu.VMEM((4, HALF, 256), F32),
            pltpu.SemaphoreType.DMA((4,)),
        ],
        compiler_params=pltpu.CompilerParams(vmem_limit_bytes=24 * 1024 * 1024),
        cost_estimate=pl.CostEstimate(flops=2_500_000_000, bytes_accessed=3_000_000, transcendentals=0),
        name="inverse",
    )(*args)


def place_rows(left, place):
    freq = jnp.arange(256, dtype=jnp.int32)
    freq = jnp.where(freq < HALF, freq, jnp.where(freq == HALF, -HALF, HALF - freq))
    eighths = freq * place
    cos_q, sin_q = (x.astype(BF16) for x in quarter(jnp.right_shift(eighths, 1)))
    base = jnp.where(jnp.bitwise_and(eighths, 1) == 1, left[1], left[0])
    c, s = base[0] * cos_q - base[1] * sin_q, base[1] * cos_q + base[0] * sin_q
    return jnp.concatenate([jnp.concatenate([c, -s], 1), jnp.concatenate([s, c], 1)], 0)


def ring(x, k):
    return lax.ppermute(x, "src", [(i, (i + k) % 4) for i in range(4)])


def body(mask_clip, source_shifts, source_weights):
    table = forward_tables()
    left, right, spread, sine = inverse_tables()
    place = lax.axis_index("row") * 4 + lax.axis_index("src")
    left_mine = place_rows(jnp.asarray(left, BF16), place)
    far, after, before, keep = forward(
        mask_clip,
        source_shifts.T,
        source_weights,
        jnp.asarray(table[:256].T, BF16),
        jnp.asarray(table, BF16),
    )
    parts = [keep, ring(far, 2), ring(before, 3), ring(after, 1)]
    summed = small(add_kernel, "add", *parts)
    mine = small(finish_kernel, "finish", summed, lax.ppermute(summed, "row", [(0, 1), (1, 0)]))
    other = lax.ppermute(mine, "src", [(0, 1), (1, 0), (2, 3), (3, 2)])
    pupil, right, spread = pupils(parts, jnp.asarray(right, BF16), jnp.asarray(spread, BF16))
    return inverse(mine, other, *parts, pupil, left_mine, right, spread, jnp.asarray(sine, F32))


def solution(mesh):
    placed = (P(("clip", "row"), "src"), P("src", None), P("src"))
    return jax.shard_map(
        body, mesh=mesh, in_specs=placed, out_specs=P(("clip", "row", "src"), None), check_vma=False
    )
```
